8 devices in a mesh: dp: 1 (over z), tp: 2 (over y), cp: 4 (over x, core).
Axes of the slice: x: 2, y: 2, z: 1, core: 2. Of those that a mesh axis runs over, the one named last changes fastest.
Arguments:
- x: bfloat16 [2048, 8192], P(('dp', 'cp'))
- doc_id: int32 [2048], P(('dp', 'cp'))
- pos_in_doc: int32 [2048], P(('dp', 'cp'))
- norm_gain: float32 [8192], replicated
- w_q: bfloat16 [8192, 8192], P(None, 'tp')
- w_k: bfloat16 [8192, 1024], P(None, 'tp')
- w_v: bfloat16 [8192, 1024], P(None, 'tp')
- w_o: bfloat16 [8192, 8192], P('tp')
- inv_freq: float32 [64], replicated
Outputs:
- output 1: bfloat16 [2048, 8192], P(('dp', 'cp'))
- output 2: bfloat16 [2048, 8, 128], P(('dp', 'cp'), 'tp')
- output 3: bfloat16 [2048, 8, 128], P(('dp', 'cp'), 'tp')
All inputs are finite; a program needn't handle non-finite values.
Results may differ from the reference program's by a relative error of at most 0.00419103.
Values are sent between devices in bfloat16 or wider.
A program may use at most 1 GiB of HBM per device.

```python
import jax
import jax.numpy as jnp
from jax import lax

TOKENS = 2048
CP_SIZE = 4
D_MODEL = 8192
Q_HEADS = 64
KV_HEADS = 8
HEAD_DIM = 128
DOC_LEN = 96
ROPE_THETA = 500000
QUERY_ROWS = 128

PIECE_LEN = TOKENS // (2 * CP_SIZE)
GROUP_SIZE = Q_HEADS // KV_HEADS
MAX_DOCS = TOKENS // (DOC_LEN // 2) + 2


def to_stored(glob_arr):
    pieces = glob_arr.reshape((2 * CP_SIZE, PIECE_LEN) + glob_arr.shape[1:])
    paired = jnp.stack([pieces[:CP_SIZE], pieces[CP_SIZE:][::-1]], axis=1)
    return paired.reshape(glob_arr.shape)


def draw_documents(doc_key):
    key_long, key_before, key_after = jax.random.split(doc_key, 3)
    first_piece = (DOC_LEN - 2) // PIECE_LEN + 1
    long_piece = jax.random.randint(key_long, (), first_piece, 2 * CP_SIZE)
    long_start = long_piece * PIECE_LEN - DOC_LEN + 1
    long_end = long_start + DOC_LEN
    lens_before = jax.random.randint(key_before, (MAX_DOCS,), DOC_LEN // 2, DOC_LEN + 1)
    lens_after = jax.random.randint(key_after, (MAX_DOCS,), DOC_LEN // 2, DOC_LEN + 1)
    starts_before = jnp.cumsum(lens_before)
    starts_after = long_end + jnp.cumsum(lens_after) - lens_after
    start_marks = jnp.zeros((TOKENS,), jnp.int32).at[0].set(1).at[long_start].set(1)
    start_marks = start_marks.at[jnp.where(starts_before < long_start, starts_before, TOKENS)].set(1, mode='drop')
    start_marks = start_marks.at[starts_after].set(1, mode='drop')
    doc_glob = jnp.cumsum(start_marks) - 1
    tok_index = jnp.arange(TOKENS)
    pos_glob = tok_index - lax.cummax(tok_index * start_marks, axis=0)
    return doc_glob.astype(jnp.int32), pos_glob.astype(jnp.int32)


def normal_weight(weight_key, fan_in, fan_out):
    return (jax.random.normal(weight_key, (fan_in, fan_out), jnp.float32) * fan_in ** -0.5).astype(jnp.bfloat16)


def setup_inputs(seed: int = 0, part: int = 0) -> dict:
    part_key = jax.random.fold_in(jax.random.key(seed), part)
    key_doc, key_noise, key_drift = jax.random.split(part_key, 3)
    shared = jax.random.split(jax.random.key(seed + 1), 6)
    doc_glob, pos_glob = draw_documents(key_doc)
    pos_ratio = pos_glob.astype(jnp.float32) / DOC_LEN
    drift_dir = jax.random.normal(key_drift, (D_MODEL,), jnp.float32)
    x_noise = jax.random.normal(key_noise, (TOKENS, D_MODEL), jnp.float32)
    x_glob = x_noise + 3.0 * pos_ratio[:, None] * drift_dir[None, :]
    norm_gain = 1.0 + 0.25 * jax.random.normal(shared[0], (D_MODEL,), jnp.float32)
    w_q = normal_weight(shared[1], D_MODEL, Q_HEADS * HEAD_DIM)
    w_k = normal_weight(shared[2], D_MODEL, KV_HEADS * HEAD_DIM)
    w_v = normal_weight(shared[3], D_MODEL, KV_HEADS * HEAD_DIM)
    w_o = normal_weight(shared[4], Q_HEADS * HEAD_DIM, D_MODEL)
    base_freq = ROPE_THETA ** (-jnp.arange(0, HEAD_DIM, 2, dtype=jnp.float32) / HEAD_DIM)
    inv_freq = base_freq * jnp.exp(0.1 * jax.random.normal(shared[5], (HEAD_DIM // 2,), jnp.float32))
    return {'x': to_stored(x_glob).astype(jnp.bfloat16), 'doc_id': to_stored(doc_glob), 'pos_in_doc': to_stored(pos_glob), 'norm_gain': norm_gain, 'w_q': w_q, 'w_k': w_k, 'w_v': w_v, 'w_o': w_o, 'inv_freq': inv_freq}


def apply_rope(vectors, cos_t, sin_t):
    half_dim = vectors.shape[-1] // 2
    lower_half = vectors[..., :half_dim].astype(jnp.float32)
    upper_half = vectors[..., half_dim:].astype(jnp.float32)
    turned = jnp.concatenate([lower_half * cos_t - upper_half * sin_t, upper_half * cos_t + lower_half * sin_t], axis=-1)
    return turned.astype(jnp.bfloat16)


def reference(x, doc_id, pos_in_doc, norm_gain, w_q, w_k, w_v, w_o, inv_freq):
    x_f32 = x.astype(jnp.float32)
    inv_rms = lax.rsqrt(jnp.mean(x_f32 * x_f32, axis=-1, keepdims=True) + 1e-5)
    normed = (x_f32 * inv_rms * norm_gain).astype(jnp.bfloat16)
    q_new = jnp.dot(normed, w_q, preferred_element_type=jnp.float32).astype(jnp.bfloat16).reshape(TOKENS, KV_HEADS, GROUP_SIZE, HEAD_DIM)
    k_new = jnp.dot(normed, w_k, preferred_element_type=jnp.float32).astype(jnp.bfloat16).reshape(TOKENS, KV_HEADS, HEAD_DIM)
    v_new = jnp.dot(normed, w_v, preferred_element_type=jnp.float32).astype(jnp.bfloat16).reshape(TOKENS, KV_HEADS, HEAD_DIM)
    rope_angle = pos_in_doc.astype(jnp.float32)[:, None] * inv_freq[None, :]
    cos_t = jnp.cos(rope_angle)
    sin_t = jnp.sin(rope_angle)
    q_rot = apply_rope(q_new, cos_t[:, None, None, :], sin_t[:, None, None, :])
    k_rot = apply_rope(k_new, cos_t[:, None, :], sin_t[:, None, :])
    tok_index = to_stored(jnp.arange(TOKENS))
    k_f32 = k_rot.astype(jnp.float32)
    v_f32 = v_new.astype(jnp.float32)
    blocks = TOKENS // QUERY_ROWS

    def attend(block_args):
        q_blk, doc_blk, idx_blk = block_args
        scores = jnp.einsum('qngd,knd->ngqk', q_blk.astype(jnp.float32), k_f32) * (HEAD_DIM ** -0.5)
        visible = (doc_blk[:, None] == doc_id[None, :]) & (tok_index[None, :] <= idx_blk[:, None])
        scores = jnp.where(visible, scores, -1e30)
        attn_probs = jax.nn.softmax(scores, axis=-1).astype(jnp.bfloat16).astype(jnp.float32)
        return jnp.einsum('ngqk,knd->qngd', attn_probs, v_f32).astype(jnp.bfloat16)

    attn_out = lax.map(attend, (q_rot.reshape(blocks, QUERY_ROWS, KV_HEADS, GROUP_SIZE, HEAD_DIM), doc_id.reshape(blocks, QUERY_ROWS), tok_index.reshape(blocks, QUERY_ROWS)))
    mixed_out = jnp.dot(attn_out.reshape(TOKENS, Q_HEADS * HEAD_DIM), w_o, preferred_element_type=jnp.float32)
    y_out = (x_f32 + mixed_out).astype(jnp.bfloat16)
    return (y_out, k_rot, v_new)
```

```python
import functools

import jax
import jax.numpy as jnp
from jax import lax
from jax.experimental import pallas as pl
from jax.experimental.pallas import tpu as pltpu
from jax.sharding import PartitionSpec as P


F32 = jnp.float32
BF16 = jnp.bfloat16
HEAD = 128
LANES = 128
VMEM_BYTES = 60 * 1024 * 1024
CHUNKS = 4


def any_spec():
    return pl.BlockSpec(memory_space=pl.ANY)


def rope_head(vec, cos_t, sin_t):
    vec = vec.astype(BF16).astype(F32)
    return (vec * cos_t + pltpu.roll(vec, HEAD // 2, 1) * sin_t).astype(BF16)


def norm_kv_kernel(half, rows, x_hbm, gain_ref, cos_ref, sin_ref, wk_hbm, wv_hbm, h_ref, kv_ref, x_buf, w_buf, x_sem, w_sem):
    d_model = x_hbm.shape[1]
    kv_cols = wk_hbm.shape[1]
    bn = w_buf.shape[2]
    per = kv_cols // bn
    nx = 4
    xr = rows // nx
    x_copies = [pltpu.make_async_copy(x_hbm.at[pl.ds(half * rows + i * xr, xr)], x_buf.at[pl.ds(i * xr, xr)], x_sem.at[i]) for i in range(nx)]
    w_copies = [pltpu.make_async_copy((wk_hbm if b < per else wv_hbm).at[:, pl.ds((b % per) * bn, bn)], w_buf.at[b], w_sem.at[b]) for b in range(2 * per)]
    for copy in x_copies + w_copies:
        copy.start()
    step = 32
    for i in range(nx):
        x_copies[i].wait()

        def body(r, carry):
            at = pl.ds(pl.multiple_of(i * xr + r * step, step), step)
            total = jnp.zeros((step, LANES), F32)
            for c in range(d_model // LANES):
                v = x_buf[at, c * LANES:(c + 1) * LANES].astype(F32)
                total += v * v
            inv = lax.rsqrt(jnp.sum(total, axis=1, keepdims=True) / d_model + 1e-5)
            for c in range(d_model // LANES):
                cols = slice(c * LANES, (c + 1) * LANES)
                h_ref[at, cols] = (x_buf[at, cols].astype(F32) * inv * gain_ref[:, cols]).astype(BF16)
            return carry

        lax.fori_loop(0, xr // step, body, 0)
    for b in range(2 * per):
        w_copies[b].wait()
        acc = jnp.dot(h_ref[...], w_buf[b], preferred_element_type=F32)
        if b < per:
            for g in range(bn // HEAD):
                cols = slice(g * HEAD, (g + 1) * HEAD)
                kv_ref[:, b * bn + g * HEAD:b * bn + (g + 1) * HEAD] = rope_head(acc[:, cols], cos_ref[...], sin_ref[...])
        else:
            kv_ref[:, b * bn:(b + 1) * bn] = acc.astype(BF16)


def norm_kv(half, rows, x_in, gain, cos_t, sin_t, w_k, w_v, deps):
    d_model = x_in.shape[1]
    kv_cols = w_k.shape[1]
    bn = 256
    blocks = 2 * kv_cols // bn
    table = pl.BlockSpec((rows, HEAD), lambda i: (half, 0))

    def kernel(x_hbm, gain_ref, cos_ref, sin_ref, wk_hbm, wv_hbm, *rest):
        norm_kv_kernel(half, rows, x_hbm, gain_ref, cos_ref, sin_ref, wk_hbm, wv_hbm, *rest[len(deps):])

    return pl.pallas_call(
        kernel,
        grid=(1,),
        in_specs=[any_spec(), pl.BlockSpec((1, d_model), lambda i: (0, 0)), table, table, any_spec(), any_spec()] + [any_spec()] * len(deps),
        out_specs=[pl.BlockSpec((rows, d_model), lambda i: (0, 0)), pl.BlockSpec((rows, 2 * kv_cols), lambda i: (0, 0))],
        out_shape=[jax.ShapeDtypeStruct((rows, d_model), BF16), jax.ShapeDtypeStruct((rows, 2 * kv_cols), BF16)],
        scratch_shapes=[
            pltpu.VMEM((rows, d_model), BF16),
            pltpu.VMEM((blocks, d_model, bn), BF16),
            pltpu.SemaphoreType.DMA((4,)),
            pltpu.SemaphoreType.DMA((blocks,)),
        ],
        compiler_params=pltpu.CompilerParams(vmem_limit_bytes=VMEM_BYTES),
        cost_estimate=pl.CostEstimate(flops=4 * rows * d_model * kv_cols, bytes_accessed=4 * d_model * (rows + kv_cols), transcendentals=0),
        name="norm_kv",
    )(x_in, gain, cos_t, sin_t, w_k, w_v, *deps)


def q_proj(half, rows, h, cos_t, sin_t, w_q, deps):
    d_model = h.shape[1]
    q_cols = w_q.shape[1]
    bn = 512
    table = pl.BlockSpec((rows, HEAD), lambda i: (half, 0))

    def kernel(h_ref, cos_ref, sin_ref, w_ref, *rest):
        q_ref = rest[-1]
        acc = jnp.dot(h_ref[...], w_ref[...], preferred_element_type=F32)
        for g in range(bn // HEAD):
            cols = slice(g * HEAD, (g + 1) * HEAD)
            q_ref[:, cols] = rope_head(acc[:, cols], cos_ref[...], sin_ref[...])

    return pl.pallas_call(
        kernel,
        grid=(q_cols // bn,),
        in_specs=[pl.BlockSpec((rows, d_model), lambda i: (0, 0)), table, table, pl.BlockSpec((d_model, bn), lambda i: (0, i))] + [any_spec()] * len(deps),
        out_specs=pl.BlockSpec((rows, bn), lambda i: (0, i)),
        out_shape=jax.ShapeDtypeStruct((rows, q_cols), BF16),
        compiler_params=pltpu.CompilerParams(vmem_limit_bytes=VMEM_BYTES),
        cost_estimate=pl.CostEstimate(flops=2 * rows * d_model * q_cols, bytes_accessed=2 * d_model * (rows + q_cols), transcendentals=0),
        name="q_proj",
    )(h, cos_t, sin_t, w_q, *deps)


def attention(half, rows, cp_size, me, pos, q, pos_col, kv_parts):
    kv_heads = kv_parts[0][0].shape[1] // (2 * HEAD)
    group = q.shape[1] // (kv_heads * HEAD)
    qb = 128
    kb = 128
    pieces = cp_size * (1 + half)
    scale = HEAD ** -0.5
    flat = [part for parts in kv_parts[:1 + half] for part in parts]

    def kernel(me_ref, pos_ref, q_ref, pos_col_ref, *rest):
        k_refs = rest[:len(flat)]
        v_refs = rest[len(flat):2 * len(flat)]
        o_ref, k_all, v_all, m_ref, l_ref, acc_ref = rest[2 * len(flat):]
        dev = me_ref[0]
        step = pl.program_id(1)

        @pl.when(step == 0)
        def _():
            for n in range(len(flat)):
                owner = lax.bitwise_xor(dev, n % cp_size)
                piece = owner if n < cp_size else 2 * cp_size - 1 - owner
                at = pl.ds(pl.multiple_of(piece * rows, rows), rows)
                k_all[at, :] = k_refs[n][...]
                v_all[at, :] = v_refs[n][...]

        piece = dev if half == 0 else 2 * cp_size - 1 - dev
        t0 = piece * rows + step * qb
        p0 = pos_ref[half * rows + step * qb]
        t_idx = t0 + lax.broadcasted_iota(jnp.int32, (qb, LANES), 0)
        first = t_idx - pos_col_ref[...]
        lane = lax.broadcasted_iota(jnp.int32, (qb, kb), 1)

        def scores(g, at):
            s = lax.dot_general(q_ref[:, g * HEAD:(g + 1) * HEAD], k_all[at, :], (((1,), (1,)), ((), ())), preferred_element_type=F32)
            return s * scale

        @pl.when(p0 <= kb)
        def _():
            w0 = pl.multiple_of(jnp.maximum(t0 - kb, 0), kb)
            at = pl.ds(w0, 2 * kb)
            u_lo = w0 + lane
            u_hi = u_lo + kb
            visible = jnp.concatenate([(u_lo >= first) & (u_lo <= t_idx), (u_hi >= first) & (u_hi <= t_idx)], axis=1)
            for g in range(group):
                s = jnp.where(visible, scores(g, at), -1e30)
                e = jnp.exp(s - jnp.max(s, axis=1, keepdims=True))
                p = (e / jnp.sum(e, axis=1, keepdims=True)).astype(BF16)
                o = jnp.dot(p, v_all[at, :], preferred_element_type=F32)
                o_ref[:, g * HEAD:(g + 1) * HEAD] = o.astype(BF16)

        @pl.when(p0 > kb)
        def _():
            kb0 = lax.div(t0 - p0, kb)
            kb1 = lax.div(t0, kb) + 1
            m_ref[...] = jnp.full_like(m_ref, -1e30)
            l_ref[...] = jnp.zeros_like(l_ref)
            acc_ref[...] = jnp.zeros_like(acc_ref)

            def masked(g, b):
                at = pl.ds(pl.multiple_of(b * kb, kb), kb)
                u = b * kb + lane
                return jnp.where((u >= first) & (u <= t_idx), scores(g, at), -1e30), at

            def stats(b, carry):
                for g in range(group):
                    s, _ = masked(g, b)
                    m_old = m_ref[g]
                    m_new = jnp.maximum(m_old, jnp.max(s, axis=1, keepdims=True))
                    l_ref[g] = l_ref[g] * jnp.exp(m_old - m_new) + jnp.sum(jnp.exp(s - m_new), axis=1, keepdims=True)
                    m_ref[g] = m_new
                return carry

            def weigh(b, carry):
                for g in range(group):
                    s, at = masked(g, b)
                    p = (jnp.exp(s - m_ref[g]) / l_ref[g]).astype(BF16)
                    acc_ref[g] += jnp.dot(p, v_all[at, :], preferred_element_type=F32)
                return carry

            lax.fori_loop(kb0, kb1, stats, 0)
            lax.fori_loop(kb0, kb1, weigh, 0)
            for g in range(group):
                o_ref[:, g * HEAD:(g + 1) * HEAD] = acc_ref[g].astype(BF16)

    q_spec = pl.BlockSpec((qb, group * HEAD), lambda n, b, *_: (b, n))
    k_specs = [pl.BlockSpec((rows, HEAD), lambda n, b, *_: (0, n))] * len(flat)
    v_specs = [pl.BlockSpec((rows, HEAD), lambda n, b, *_: (0, kv_heads + n))] * len(flat)
    keys = pieces * rows
    return pl.pallas_call(
        kernel,
        grid_spec=pltpu.PrefetchScalarGridSpec(
            num_scalar_prefetch=2,
            grid=(kv_heads, rows // qb),
            in_specs=[q_spec, pl.BlockSpec((qb, LANES), lambda n, b, *_: (half * (rows // qb) + b, 0))] + k_specs + v_specs,
            out_specs=q_spec,
            scratch_shapes=[
                pltpu.VMEM((keys, HEAD), BF16),
                pltpu.VMEM((keys, HEAD), BF16),
                pltpu.VMEM((group, qb, LANES), F32),
                pltpu.VMEM((group, qb, LANES), F32),
                pltpu.VMEM((group, qb, HEAD), F32),
            ],
        ),
        out_shape=jax.ShapeDtypeStruct(q.shape, BF16),
        compiler_params=pltpu.CompilerParams(vmem_limit_bytes=VMEM_BYTES),
        cost_estimate=pl.CostEstimate(flops=4 * rows * q.shape[1] * 512, bytes_accessed=8 * rows * q.shape[1], transcendentals=0),
        name="attend",
    )(me, pos, q, pos_col, *flat, *flat)


def out_send(rows, tp_me, o, w_o, chunk, cols, deps):
    k_dim = o.shape[1]
    bn = 256
    own_blocks = w_o.shape[1] // 2 // bn

    def kernel(tp_ref, o_ref, w_ref, *rest):
        rest[-1][...] = jnp.dot(o_ref[...], w_ref[...], preferred_element_type=F32)

    return pl.pallas_call(
        kernel,
        grid_spec=pltpu.PrefetchScalarGridSpec(
            num_scalar_prefetch=1,
            grid=(cols // bn,),
            in_specs=[pl.BlockSpec((rows, k_dim), lambda i, tp: (0, 0)), pl.BlockSpec((k_dim, bn), lambda i, tp: (0, (1 - tp[0]) * own_blocks + chunk * (cols // bn) + i))] + [any_spec()] * len(deps),
            out_specs=pl.BlockSpec((rows, bn), lambda i, tp: (0, i)),
        ),
        out_shape=jax.ShapeDtypeStruct((rows, cols), F32),
        compiler_params=pltpu.CompilerParams(vmem_limit_bytes=VMEM_BYTES),
        cost_estimate=pl.CostEstimate(flops=2 * rows * k_dim * cols, bytes_accessed=2 * k_dim * (rows + cols), transcendentals=0),
        name="out_send",
    )(tp_me, o, w_o, *deps)


def out_own(half, rows, tp_me, o, w_o, x_in, recv, y_buf, chunk, cols, deps):
    k_dim = o.shape[1]
    bn = 256
    own_blocks = w_o.shape[1] // 2 // bn

    def col(i, tp):
        return tp[0] * own_blocks + chunk * (cols // bn) + i

    def kernel(tp_ref, o_ref, w_ref, x_ref, r_ref, *rest):
        y_ref, c_ref = rest[-2:]
        acc = jnp.dot(o_ref[...], w_ref[...], preferred_element_type=F32)
        out = (x_ref[...].astype(F32) + (acc + r_ref[...])).astype(BF16)
        y_ref[...] = out
        c_ref[...] = out

    ins = [o, w_o, x_in, recv] + ([] if y_buf is None else [y_buf]) + list(deps)
    wide = pl.BlockSpec((rows, bn), lambda i, tp: (half, col(i, tp)))
    narrow = pl.BlockSpec((rows, bn), lambda i, tp: (0, i))
    return pl.pallas_call(
        kernel,
        grid_spec=pltpu.PrefetchScalarGridSpec(
            num_scalar_prefetch=1,
            grid=(cols // bn,),
            in_specs=[pl.BlockSpec((rows, k_dim), lambda i, tp: (0, 0)), pl.BlockSpec((k_dim, bn), lambda i, tp: (0, col(i, tp))), wide, narrow] + [any_spec()] * (len(ins) - 4),
            out_specs=[wide, narrow],
        ),
        out_shape=[jax.ShapeDtypeStruct(x_in.shape, BF16), jax.ShapeDtypeStruct((rows, cols), BF16)],
        input_output_aliases={} if y_buf is None else {5: 0},
        compiler_params=pltpu.CompilerParams(vmem_limit_bytes=VMEM_BYTES),
        cost_estimate=pl.CostEstimate(flops=2 * rows * k_dim * cols, bytes_accessed=2 * k_dim * (rows + cols), transcendentals=0),
        name="out_own",
    )(tp_me, *ins)


def place(half, rows, tp_me, recv, y_buf, chunk, cols):
    own_blocks = y_buf.shape[1] // 2 // cols

    def kernel(tp_ref, r_ref, y_in, y_ref):
        y_ref[...] = r_ref[...]

    return pl.pallas_call(
        kernel,
        grid_spec=pltpu.PrefetchScalarGridSpec(
            num_scalar_prefetch=1,
            grid=(1,),
            in_specs=[pl.BlockSpec((rows, cols), lambda i, tp: (0, 0)), any_spec()],
            out_specs=pl.BlockSpec((rows, cols), lambda i, tp: (half, (1 - tp[0]) * own_blocks + chunk)),
        ),
        out_shape=jax.ShapeDtypeStruct(y_buf.shape, BF16),
        input_output_aliases={2: 0},
        cost_estimate=pl.CostEstimate(flops=rows * cols, bytes_accessed=4 * rows * cols, transcendentals=0),
        name="place",
    )(tp_me, recv, y_buf)


def solution(mesh):
    cp_size = mesh.shape['cp']
    tp_size = mesh.shape['tp']
    swap_tp = [(j, tp_size - 1 - j) for j in range(tp_size)]

    def local_step(x_in, doc_id, pos_in_doc, norm_gain, w_q, w_k, w_v, w_o, inv_freq):
        local_rows, d_model = x_in.shape
        rows = local_rows // 2
        kv_cols = w_k.shape[1]
        me = lax.axis_index('cp').astype(jnp.int32).reshape(1)
        tp_me = lax.axis_index('tp').astype(jnp.int32).reshape(1)
        angle = pos_in_doc.astype(F32)[:, None] * inv_freq[None, :]
        cos_h, sin_h = jnp.cos(angle), jnp.sin(angle)
        cos_t = jnp.concatenate([cos_h, cos_h], axis=1)
        sin_t = jnp.concatenate([-sin_h, sin_h], axis=1)
        gain = norm_gain.reshape(1, d_model)
        pos_col = jnp.broadcast_to(pos_in_doc[:, None], (local_rows, LANES))
        cols = d_model // 2 // CHUNKS

        kv_parts, sent, attn = [], [], []
        deps = ()
        for half in range(2):
            h, kv = norm_kv(half, rows, x_in, gain, cos_t, sin_t, w_k, w_v, deps)
            parts = [kv]
            for d in range(1, cp_size):
                parts.append(lax.ppermute(kv, 'cp', [(i, i ^ d) for i in range(cp_size)]))
            kv_parts.append(parts)
            q = q_proj(half, rows, h, cos_t, sin_t, w_q, ())
            o = attention(half, rows, cp_size, me, pos_in_doc, q, pos_col, kv_parts)
            attn.append(o)
            deps = ()
            for c in range(CHUNKS):
                part = out_send(rows, tp_me, o, w_o, c, cols, deps)
                deps = (part,)
                sent.append(lax.ppermute(part, 'tp', swap_tp))

        y_buf = None
        results = []
        for half in range(2):
            for c in range(CHUNKS):
                y_buf, block = out_own(half, rows, tp_me, attn[half], w_o, x_in, sent[half * CHUNKS + c], y_buf, c, cols, deps)
                results.append(lax.ppermute(block, 'tp', swap_tp))
        for half in range(2):
            for c in range(CHUNKS):
                y_buf = place(half, rows, tp_me, results[half * CHUNKS + c], y_buf, c, cols)
        kv_all = jnp.concatenate([parts[0] for parts in kv_parts], axis=0)
        k_out = kv_all[:, :kv_cols].reshape(local_rows, kv_cols // HEAD, HEAD)
        v_out = kv_all[:, kv_cols:].reshape(local_rows, kv_cols // HEAD, HEAD)
        return y_buf, k_out, v_out

    row_spec = P(('dp', 'cp'))
    in_specs = (P(('dp', 'cp'), None), row_spec, row_spec, P(), P(None, 'tp'), P(None, 'tp'), P(None, 'tp'), P('tp', None), P())
    out_specs = (P(('dp', 'cp'), None), P(('dp', 'cp'), 'tp', None), P(('dp', 'cp'), 'tp', None))
    return jax.shard_map(local_step, mesh=mesh, in_specs=in_specs, out_specs=out_specs, check_vma=False)
```

```python
import jax
import jax.numpy as jnp
from jax import lax
from jax.experimental import pallas as pl
from jax.experimental.pallas import tpu as pltpu
from jax.sharding import PartitionSpec as P


F32 = jnp.float32
BF16 = jnp.bfloat16
HEAD = 128
LANES = 128
VMEM_BYTES = 60 * 1024 * 1024
CHUNKS = ((512, 1024, 1024, 1536), (1536, 1024, 1024, 512))


def any_spec():
    return pl.BlockSpec(memory_space=pl.ANY)


def rope_head(vec, cos_t, sin_t):
    vec = vec.astype(BF16).astype(F32)
    return (vec * cos_t + pltpu.roll(vec, HEAD // 2, 1) * sin_t).astype(BF16)


def front(half, rows, x_in, gain, pos2, inv_freq, w_q, w_k, w_v):
    d_model = x_in.shape[1]
    kv_cols = w_k.shape[1]
    q_cols = w_q.shape[1]
    bn = kv_cols
    nq = q_cols // bn
    slots = 4
    nx = 4
    xr = rows // nx
    step = 32

    def kernel(x_hbm, gain_ref, pos_ref, freq_ref, wk_hbm, wv_hbm, wq_hbm, q_hbm, kv_ref, r1, r2, r3, x_buf, h_ref, ring, q_buf, cos_ref, sin_ref, freq2_ref, x_sem, w_sem, q_sem, s_sem, r_sem):
        me = lax.axis_index('cp')
        core, across = lax.bitwise_xor(me, 1), lax.bitwise_xor(me, 2)
        barrier = pltpu.get_barrier_semaphore()
        for peer in (core, across):
            pl.semaphore_signal(barrier, inc=1, device_id={'cp': peer}, device_id_type=pl.DeviceIdType.MESH)
        x_copies = [pltpu.make_async_copy(x_hbm.at[pl.ds(half * rows + i * xr, xr)], x_buf.at[pl.ds(i * xr, xr)], x_sem.at[i]) for i in range(nx)]
        for copy in x_copies:
            copy.start()

        def q_load(b):
            slot = lax.rem(b + 2, slots)
            return pltpu.make_async_copy(wq_hbm.at[:, pl.ds(pl.multiple_of(b * bn, bn), bn)], ring.at[slot], w_sem.at[slot])

        kv_loads = [pltpu.make_async_copy(wk_hbm, ring.at[0], w_sem.at[0]), pltpu.make_async_copy(wv_hbm, ring.at[1], w_sem.at[1])]
        for load in kv_loads:
            load.start()
        for b in range(slots - 2):
            q_load(b).start()

        half_dim = HEAD // 2
        freq2_ref[:, :half_dim] = freq_ref[...]
        freq2_ref[:, half_dim:] = freq_ref[...]
        sign = jnp.where(lax.broadcasted_iota(jnp.int32, (LANES, HEAD), 1) < half_dim, -1.0, 1.0)
        for b in range(rows // LANES):
            pos_row = pos_ref[half * (rows // LANES) + b:half * (rows // LANES) + b + 1, :].astype(F32)
            angle = jnp.transpose(jnp.broadcast_to(pos_row, (LANES, LANES))) * freq2_ref[...]
            cos_ref[b * LANES:(b + 1) * LANES, :] = jnp.cos(angle)
            sin_ref[b * LANES:(b + 1) * LANES, :] = jnp.sin(angle) * sign

        for i in range(nx):
            x_copies[i].wait()

            def norm(r, carry):
                at = pl.ds(pl.multiple_of(i * xr + r * step, step), step)
                total = jnp.zeros((step, LANES), F32)
                for c in range(d_model // LANES):
                    v = x_buf[at, c * LANES:(c + 1) * LANES].astype(F32)
                    total += v * v
                inv = lax.rsqrt(jnp.sum(total, axis=1, keepdims=True) / d_model + 1e-5)
                for c in range(d_model // LANES):
                    cols = slice(c * LANES, (c + 1) * LANES)
                    h_ref[at, cols] = (x_buf[at, cols].astype(F32) * inv * gain_ref[:, cols]).astype(BF16)
                return carry

            lax.fori_loop(0, xr // step, norm, 0)

        kv_loads[0].wait()
        acc = jnp.dot(h_ref[...], ring[0], preferred_element_type=F32)
        for g in range(bn // HEAD):
            cols = slice(g * HEAD, (g + 1) * HEAD)
            kv_ref[:, cols] = rope_head(acc[:, cols], cos_ref[...], sin_ref[...])
        q_load(slots - 2).start()
        kv_loads[1].wait()
        kv_ref[:, kv_cols:] = jnp.dot(h_ref[...], ring[1], preferred_element_type=F32).astype(BF16)
        q_load(slots - 1).start()

        pl.semaphore_wait(barrier, 2)
        sends = []
        for n, (dst, peer) in enumerate(((r2, across), (r1, core))):
            sends.append(pltpu.make_async_remote_copy(src_ref=kv_ref, dst_ref=dst, send_sem=s_sem.at[n], recv_sem=r_sem.at[n], device_id={'cp': peer}, device_id_type=pl.DeviceIdType.MESH))
            sends[-1].start()
        forward = pltpu.make_async_remote_copy(src_ref=r2, dst_ref=r3, send_sem=s_sem.at[2], recv_sem=r_sem.at[2], device_id={'cp': core}, device_id_type=pl.DeviceIdType.MESH)

        def q_store(b):
            cols = pl.ds(pl.multiple_of(b * bn, bn), bn)
            return pltpu.make_async_copy(q_buf.at[:, cols], q_hbm.at[:, cols], q_sem.at[b])

        def q_block(b, carry):
            slot = lax.rem(b + 2, slots)
            q_load(b).wait()
            acc = jnp.dot(h_ref[...], ring[slot], preferred_element_type=F32)
            for g in range(bn // HEAD):
                at = pl.ds(pl.multiple_of(b * bn + g * HEAD, HEAD), HEAD)
                q_buf[:, at] = rope_head(acc[:, g * HEAD:(g + 1) * HEAD], cos_ref[...], sin_ref[...])
            q_store(b).start()

            @pl.when(b + slots < nq)
            def _():
                q_load(b + slots).start()

            return carry

        lax.fori_loop(0, nq - 2, q_block, 0)
        sends[0].wait_recv()
        forward.start()
        lax.fori_loop(nq - 2, nq, q_block, 0)
        for b in range(nq):
            q_store(b).wait()
        sends[0].wait_send()
        sends[1].wait()
        forward.wait()

    whole = lambda arr: pl.BlockSpec(arr.shape, lambda i: (0, 0))
    kv_shape = jax.ShapeDtypeStruct((rows, 2 * kv_cols), BF16)
    return pl.pallas_call(
        kernel,
        grid=(1,),
        in_specs=[any_spec(), whole(gain), whole(pos2), whole(inv_freq), any_spec(), any_spec(), any_spec()],
        out_specs=[any_spec(), pl.BlockSpec(kv_shape.shape, lambda i: (0, 0)), any_spec(), any_spec(), any_spec()],
        out_shape=[jax.ShapeDtypeStruct((rows, q_cols), BF16), kv_shape, kv_shape, kv_shape, kv_shape],
        scratch_shapes=[
            pltpu.VMEM((rows, d_model), BF16),
            pltpu.VMEM((rows, d_model), BF16),
            pltpu.VMEM((slots, d_model, bn), BF16),
            pltpu.VMEM((rows, q_cols), BF16),
            pltpu.VMEM((rows, HEAD), F32),
            pltpu.VMEM((rows, HEAD), F32),
            pltpu.VMEM((1, HEAD), F32),
            pltpu.SemaphoreType.DMA((nx,)),
            pltpu.SemaphoreType.DMA((slots,)),
            pltpu.SemaphoreType.DMA((nq,)),
            pltpu.SemaphoreType.DMA((3,)),
            pltpu.SemaphoreType.DMA((3,)),
        ],
        compiler_params=pltpu.CompilerParams(vmem_limit_bytes=VMEM_BYTES, collective_id=half, has_side_effects=True),
        cost_estimate=pl.CostEstimate(flops=2 * rows * d_model * (2 * kv_cols + q_cols), bytes_accessed=2 * d_model * (rows + q_cols), transcendentals=0),
        name="front",
    )(x_in, gain, pos2, inv_freq, w_k, w_v, w_q)


def attend_send(half, rows, cp_size, ids, pos, pos2, q, kv_parts, w_o, cols):
    kv_heads = kv_parts[0].shape[1] // (2 * HEAD)
    group = q.shape[1] // (kv_heads * HEAD)
    qb = kb = 128
    steps = rows // qb
    keys = cp_size * rows * (1 + half)
    scale = HEAD ** -0.5
    parts = len(kv_parts)
    k_dim = q.shape[1]
    half_cols = w_o.shape[1] // 2

    def kernel(ids_ref, pos_ref, pos2_ref, q_hbm, w_hbm, *rest):
        kv_hbm = rest[:parts]
        o_ref, part_ref, kv_all, q_buf, w_buf, s_ref, p_ref, m_ref, l_ref, acc_ref, kv_sem, q_sem, w_sem = rest[parts:]
        dev, tp = ids_ref[0], ids_ref[1]
        copies = []
        for n in range(parts):
            owner = lax.bitwise_xor(dev, n % cp_size)
            piece = owner if n < cp_size else 2 * cp_size - 1 - owner
            copies.append(pltpu.make_async_copy(kv_hbm[n], kv_all.at[pl.ds(pl.multiple_of(piece * rows, rows), rows)], kv_sem.at[n]))
            copies[-1].start()

        def q_copy(n):
            at = pl.ds(pl.multiple_of(n * group * HEAD, group * HEAD), group * HEAD)
            return pltpu.make_async_copy(q_hbm.at[:, at], q_buf.at[:, at], q_sem.at[n])

        for n in range(kv_heads):
            q_copy(n).start()
        w_copy = pltpu.make_async_copy(w_hbm.at[:, pl.ds(pl.multiple_of((1 - tp) * half_cols, half_cols), cols)], w_buf, w_sem)
        w_copy.start()
        for c in copies: c.wait()
        piece = dev if half == 0 else 2 * cp_size - 1 - dev
        lane = lax.broadcasted_iota(jnp.int32, (qb, LANES), 1)
        row = lax.broadcasted_iota(jnp.int32, (qb, LANES), 0)

        def step_body(i, carry):
            n, b = lax.div(i, steps), lax.rem(i, steps)

            @pl.when(b == 0)
            def _(): q_copy(n).wait()

            t0 = piece * rows + b * qb
            p0 = pos_ref[half * rows + b * qb]
            q_rows = pl.ds(pl.multiple_of(b * qb, qb), qb)

            def head_cols(g): return pl.ds(pl.multiple_of((n * group + g) * HEAD, HEAD), HEAD)

            k_cols = pl.ds(pl.multiple_of(n * HEAD, HEAD), HEAD)
            v_cols = pl.ds(pl.multiple_of((kv_heads + n) * HEAD, HEAD), HEAD)
            pos_row = pos2_ref[pl.ds(half * steps + b, 1), :].astype(F32)
            pos_t = jnp.transpose(jnp.broadcast_to(pos_row, (qb, LANES))).astype(jnp.int32)
            t_idx = t0 + row
            first = t_idx - pos_t
            q_stack = jnp.concatenate([q_buf[q_rows, head_cols(g)] for g in range(group)], axis=0)

            @pl.when(p0 <= kb)
            def _():
                w0 = pl.multiple_of(jnp.maximum(t0 - kb, 0), kb)
                at = pl.ds(w0, 2 * kb)
                s_ref[...] = lax.dot_general(q_stack, kv_all[at, k_cols], (((1,), (1,)), ((), ())), preferred_element_type=F32)
                u = w0 + lane
                see = [(u >= first) & (u <= t_idx), (u + kb >= first) & (u + kb <= t_idx)]
                visible = jnp.concatenate(see, axis=1)
                for g in range(group):
                    at_g = slice(g * qb, (g + 1) * qb)
                    s = jnp.where(visible, s_ref[at_g] * scale, -1e30)
                    s_ref[at_g] = s
                    m_ref[g] = jnp.broadcast_to(jnp.max(s, axis=1, keepdims=True), (qb, LANES))
                for g in range(group):
                    at_g = slice(g * qb, (g + 1) * qb)
                    m = m_ref[g]
                    e = jnp.exp(s_ref[at_g] - jnp.concatenate([m, m], axis=1))
                    s_ref[at_g] = e
                    l_ref[g] = 1.0 / jnp.broadcast_to(jnp.sum(e, axis=1, keepdims=True), (qb, LANES))
                for g in range(group):
                    at_g = slice(g * qb, (g + 1) * qb)
                    l = l_ref[g]
                    p_ref[at_g] = (s_ref[at_g] * jnp.concatenate([l, l], axis=1)).astype(BF16)
                o = jnp.dot(p_ref[...], kv_all[at, v_cols], preferred_element_type=F32).astype(BF16)
                for g in range(group):
                    o_ref[q_rows, head_cols(g)] = o[g * qb:(g + 1) * qb]

            @pl.when(p0 > kb)
            def _():
                kb0 = lax.div(t0 - p0, kb)
                kb1 = lax.div(t0, kb) + 1
                m_ref[...] = jnp.full_like(m_ref, -1e30)
                l_ref[...] = jnp.zeros_like(l_ref)
                acc_ref[...] = jnp.zeros_like(acc_ref)

                def block(j):
                    at = pl.ds(pl.multiple_of(j * kb, kb), kb)
                    u = j * kb + lane
                    s_ref[:, :kb] = lax.dot_general(q_stack, kv_all[at, k_cols], (((1,), (1,)), ((), ())), preferred_element_type=F32)
                    return at, (u >= first) & (u <= t_idx)

                def stats(j, carry):
                    _, visible = block(j)
                    for g in range(group):
                        s = jnp.where(visible, s_ref[g * qb:(g + 1) * qb, :kb] * scale, -1e30)
                        m_old = m_ref[g]
                        m_new = jnp.maximum(m_old, jnp.max(s, axis=1, keepdims=True))
                        l_ref[g] = l_ref[g] * jnp.exp(m_old - m_new) + jnp.sum(jnp.exp(s - m_new), axis=1, keepdims=True)
                        m_ref[g] = m_new
                    return carry

                def weigh(j, carry):
                    at, visible = block(j)
                    for g in range(group):
                        at_g = slice(g * qb, (g + 1) * qb)
                        s = jnp.where(visible, s_ref[at_g, :kb] * scale, -1e30)
                        p_ref[at_g, :kb] = (jnp.exp(s - m_ref[g]) / l_ref[g]).astype(BF16)
                    acc_ref[...] += jnp.dot(p_ref[:, :kb], kv_all[at, v_cols], preferred_element_type=F32)
                    return carry

                lax.fori_loop(kb0, kb1, stats, 0)
                lax.fori_loop(kb0, kb1, weigh, 0)
                for g in range(group):
                    o_ref[q_rows, head_cols(g)] = acc_ref[g * qb:(g + 1) * qb].astype(BF16)

            return carry

        lax.fori_loop(0, kv_heads * steps, step_body, 0)
        w_copy.wait()
        part_ref[...] = jnp.dot(o_ref[...], w_buf[...], preferred_element_type=F32)

    whole = lambda shape: pl.BlockSpec(shape, lambda i, *_: (0, 0))
    return pl.pallas_call(
        kernel,
        grid_spec=pltpu.PrefetchScalarGridSpec(
            num_scalar_prefetch=2, grid=(1,),
            in_specs=[whole(pos2.shape), any_spec(), any_spec()] + [any_spec()] * parts,
            out_specs=[whole(q.shape), whole((rows, cols))],
            scratch_shapes=[
                pltpu.VMEM((keys, kv_parts[0].shape[1]), BF16), pltpu.VMEM(q.shape, BF16), pltpu.VMEM((k_dim, cols), BF16),
                pltpu.VMEM((group * qb, 2 * kb), F32), pltpu.VMEM((group * qb, 2 * kb), BF16),
                pltpu.VMEM((group, qb, LANES), F32), pltpu.VMEM((group, qb, LANES), F32), pltpu.VMEM((group * qb, HEAD), F32),
                pltpu.SemaphoreType.DMA((parts,)), pltpu.SemaphoreType.DMA((kv_heads,)), pltpu.SemaphoreType.DMA,
            ]),
        out_shape=[jax.ShapeDtypeStruct(q.shape, BF16), jax.ShapeDtypeStruct((rows, cols), F32)],
        compiler_params=pltpu.CompilerParams(vmem_limit_bytes=VMEM_BYTES),
        cost_estimate=pl.CostEstimate(flops=4 * rows * q.shape[1] * 512 + 2 * rows * k_dim * cols, bytes_accessed=2 * k_dim * cols, transcendentals=0),
        name="attend_send")(ids, pos, pos2, q, w_o, *kv_parts)


def out_send(rows, tp_me, o, w_o, col0, cols):
    k_dim = o.shape[1]
    bn = 512
    own_blocks = w_o.shape[1] // 2 // bn

    def kernel(tp_ref, o_ref, w_ref, *rest):
        rest[-1][...] = jnp.dot(o_ref[...], w_ref[...], preferred_element_type=F32)

    return pl.pallas_call(
        kernel,
        grid_spec=pltpu.PrefetchScalarGridSpec(
            num_scalar_prefetch=1,
            grid=(cols // bn,),
            in_specs=[pl.BlockSpec((rows, k_dim), lambda i, tp: (0, 0)), pl.BlockSpec((k_dim, bn), lambda i, tp: (0, (1 - tp[0]) * own_blocks + col0 // bn + i))],
            out_specs=pl.BlockSpec((rows, bn), lambda i, tp: (0, i)),
        ),
        out_shape=jax.ShapeDtypeStruct((rows, cols), F32),
        compiler_params=pltpu.CompilerParams(vmem_limit_bytes=VMEM_BYTES),
        cost_estimate=pl.CostEstimate(flops=2 * rows * k_dim * cols, bytes_accessed=2 * k_dim * (rows + cols), transcendentals=0),
        name="out_send",
    )(tp_me, o, w_o)


def out_own(half, rows, tp_me, o, w_o, x_in, recv, y_buf, col0, cols):
    k_dim = o.shape[1]
    bn = 512
    own_blocks = w_o.shape[1] // 2 // bn

    def col(i, tp):
        return tp[0] * own_blocks + col0 // bn + i

    def kernel(tp_ref, o_ref, w_ref, x_ref, r_ref, *rest):
        y_ref, c_ref = rest[-2:]
        acc = jnp.dot(o_ref[...], w_ref[...], preferred_element_type=F32)
        out = (x_ref[...].astype(F32) + (acc + r_ref[...])).astype(BF16)
        y_ref[...] = out
        c_ref[...] = out

    ins = [o, w_o, x_in, recv] + ([] if y_buf is None else [y_buf])
    wide = pl.BlockSpec((rows, bn), lambda i, tp: (half, col(i, tp)))
    narrow = pl.BlockSpec((rows, bn), lambda i, tp: (0, i))
    return pl.pallas_call(
        kernel,
        grid_spec=pltpu.PrefetchScalarGridSpec(
            num_scalar_prefetch=1,
            grid=(cols // bn,),
            in_specs=[pl.BlockSpec((rows, k_dim), lambda i, tp: (0, 0)), pl.BlockSpec((k_dim, bn), lambda i, tp: (0, col(i, tp))), wide, narrow] + [any_spec()] * (len(ins) - 4),
            out_specs=[wide, narrow],
        ),
        out_shape=[jax.ShapeDtypeStruct(x_in.shape, BF16), jax.ShapeDtypeStruct((rows, cols), BF16)],
        input_output_aliases={} if y_buf is None else {5: 0},
        compiler_params=pltpu.CompilerParams(vmem_limit_bytes=VMEM_BYTES),
        cost_estimate=pl.CostEstimate(flops=2 * rows * k_dim * cols, bytes_accessed=2 * k_dim * (rows + cols), transcendentals=0),
        name="out_own",
    )(tp_me, *ins)


def place(half, rows, tp_me, recv, y_buf, col0, cols):
    bn = 512
    own_blocks = y_buf.shape[1] // 2 // bn

    def kernel(tp_ref, r_ref, y_in, y_ref):
        y_ref[...] = r_ref[...]

    return pl.pallas_call(
        kernel,
        grid_spec=pltpu.PrefetchScalarGridSpec(
            num_scalar_prefetch=1,
            grid=(cols // bn,),
            in_specs=[pl.BlockSpec((rows, bn), lambda i, tp: (0, i)), any_spec()],
            out_specs=pl.BlockSpec((rows, bn), lambda i, tp: (half, (1 - tp[0]) * own_blocks + col0 // bn + i)),
        ),
        out_shape=jax.ShapeDtypeStruct(y_buf.shape, BF16),
        input_output_aliases={2: 0},
        compiler_params=pltpu.CompilerParams(vmem_limit_bytes=VMEM_BYTES),
        cost_estimate=pl.CostEstimate(flops=rows * cols, bytes_accessed=4 * rows * cols, transcendentals=0),
        name="place",
    )(tp_me, recv, y_buf)


def solution(mesh):
    cp_size = mesh.shape['cp']
    tp_size = mesh.shape['tp']
    swap_tp = [(j, tp_size - 1 - j) for j in range(tp_size)]

    def local_step(x_in, doc_id, pos_in_doc, norm_gain, w_q, w_k, w_v, w_o, inv_freq):
        local_rows, d_model = x_in.shape
        rows = local_rows // 2
        kv_cols = w_k.shape[1]
        me = lax.axis_index('cp').astype(jnp.int32)
        tp_one = lax.axis_index('tp').astype(jnp.int32)
        ids = jnp.stack([me, tp_one])
        tp_me = tp_one.reshape(1)
        gain = norm_gain.reshape(1, d_model)
        pos2 = pos_in_doc.reshape(local_rows // LANES, LANES)
        freq = inv_freq.reshape(1, HEAD // 2)

        kv_parts, sent, attn = [], [], []
        for half in range(2):
            q, *parts = front(half, rows, x_in, gain, pos2, freq, w_q, w_k, w_v)
            kv_parts += parts
            sizes = CHUNKS[half]
            o, part = attend_send(half, rows, cp_size, ids, pos_in_doc, pos2, q, kv_parts, w_o, sizes[0])
            attn.append(o)
            col0 = 0
            for c, cols in enumerate(sizes):
                if c:
                    part = out_send(rows, tp_me, o, w_o, col0, cols)
                sent.append(lax.ppermute(part, 'tp', swap_tp))
                col0 += cols

        y_buf = None
        results = []
        where = [(half, sum(CHUNKS[half][:c]), cols) for half in range(2) for c, cols in enumerate(CHUNKS[half])]
        for n, (half, col0, cols) in enumerate(where):
            y_buf, block = out_own(half, rows, tp_me, attn[half], w_o, x_in, sent[n], y_buf, col0, cols)
            results.append(lax.ppermute(block, 'tp', swap_tp))
        for n, (half, col0, cols) in enumerate(where):
            y_buf = place(half, rows, tp_me, results[n], y_buf, col0, cols)
        kv_all = jnp.concatenate([kv_parts[0], kv_parts[cp_size]], axis=0)
        k_out = kv_all[:, :kv_cols].reshape(local_rows, kv_cols // HEAD, HEAD)
        v_out = kv_all[:, kv_cols:].reshape(local_rows, kv_cols // HEAD, HEAD)
        return y_buf, k_out, v_out

    row_spec = P(('dp', 'cp'))
    in_specs = (P(('dp', 'cp'), None), row_spec, row_spec, P(), P(None, 'tp'), P(None, 'tp'), P(None, 'tp'), P('tp', None), P())
    out_specs = (P(('dp', 'cp'), None), P(('dp', 'cp'), 'tp', None), P(('dp', 'cp'), 'tp', None))

    return jax.shard_map(local_step, mesh=mesh, in_specs=in_specs, out_specs=out_specs, check_vma=False)
```

```python
import jax
import jax.numpy as jnp
from jax import lax
from jax.experimental import pallas as pl
from jax.experimental.pallas import tpu as pltpu
from jax.sharding import PartitionSpec as P


F32 = jnp.float32
BF16 = jnp.bfloat16
HEAD = 128
LANES = 128
VMEM_BYTES = 60 * 1024 * 1024
ROWS = 128
CHUNKS = ((1024, 3072), (1024, 3072), (1024, 3072), (1024, 2048, 512, 512))
PLAN = (("make", 0, 0, 2), ("make", 1, 0, 2), ("own", 0, 0, 2), ("make", 2, 0, 2), ("own", 1, 0, 2), ("make", 3, 0, 4), ("own", 2, 0, 2), ("own", 3, 0, 1), ("own", 3, 1, 2), ("own", 3, 2, 3), ("own", 3, 3, 4))


def any_spec():
    return pl.BlockSpec(memory_space=pl.ANY)


def rope_head(vec, cos_t, sin_t):
    vec = vec.astype(BF16).astype(F32)
    return (vec * cos_t + pltpu.roll(vec, HEAD // 2, 1) * sin_t).astype(BF16)


def front(group, with_kv, x_in, gain, pos2, inv_freq, w_q, w_k, w_v):
    d_model = x_in.shape[1]
    kv_cols = w_k.shape[1]
    q_cols = w_q.shape[1]
    bn = kv_cols
    nq = q_cols // bn
    slots = 4
    xr = 64
    rows = 2 * ROWS if with_kv else ROWS
    nx = rows // xr
    step = 32
    lead = 2 if with_kv else 0

    def kernel(x_hbm, gain_ref, pos_ref, freq_ref, wq_hbm, *rest):
        if with_kv:
            wk_hbm, wv_hbm, q_hbm, kv_ref, r1, r2, r3 = rest[:7]
            s_sem, r_sem = rest[-2:]
            rest = rest[7:-2]
            me = lax.axis_index('cp')
            core, across = lax.bitwise_xor(me, 1), lax.bitwise_xor(me, 2)
            barrier = pltpu.get_barrier_semaphore()
            for peer in (core, across):
                pl.semaphore_signal(barrier, inc=1, device_id={'cp': peer}, device_id_type=pl.DeviceIdType.MESH)
        else:
            q_hbm = rest[0]
            rest = rest[1:]
        x_buf, h_ref, ring, q_buf, cos_ref, sin_ref, freq2_ref, x_sem, w_sem, q_sem = rest
        x_copies = [pltpu.make_async_copy(x_hbm.at[pl.ds(group * ROWS + i * xr, xr)], x_buf.at[pl.ds(i * xr, xr)], x_sem.at[i]) for i in range(nx)]
        for copy in x_copies:
            copy.start()

        def q_load(b):
            slot = lax.rem(b + lead, slots)
            return pltpu.make_async_copy(wq_hbm.at[:, pl.ds(pl.multiple_of(b * bn, bn), bn)], ring.at[slot], w_sem.at[slot])

        kv_loads = [pltpu.make_async_copy(w_hbm, ring.at[n], w_sem.at[n]) for n, w_hbm in enumerate((wk_hbm, wv_hbm))] if with_kv else []
        for load in kv_loads:
            load.start()
        for b in range(slots - lead):
            q_load(b).start()

        half_dim = HEAD // 2
        freq2_ref[:, :half_dim] = freq_ref[...]
        freq2_ref[:, half_dim:] = freq_ref[...]
        sign = jnp.where(lax.broadcasted_iota(jnp.int32, (LANES, HEAD), 1) < half_dim, -1.0, 1.0)
        for b in range(rows // LANES):
            pos_row = pos_ref[group + b:group + b + 1, :].astype(F32)
            angle = jnp.transpose(jnp.broadcast_to(pos_row, (LANES, LANES))) * freq2_ref[...]
            cos_ref[b * LANES:(b + 1) * LANES, :] = jnp.cos(angle)
            sin_ref[b * LANES:(b + 1) * LANES, :] = jnp.sin(angle) * sign

        def norm(r, carry):
            at = pl.ds(pl.multiple_of(r * step, step), step)
            total = jnp.zeros((step, LANES), F32)
            for c in range(d_model // LANES):
                v = x_buf[at, c * LANES:(c + 1) * LANES].astype(F32)
                total += v * v
            inv = lax.rsqrt(jnp.sum(total, axis=1, keepdims=True) / d_model + 1e-5)
            for c in range(d_model // LANES):
                cols = slice(c * LANES, (c + 1) * LANES)
                h_ref[at, cols] = (x_buf[at, cols].astype(F32) * inv * gain_ref[:, cols]).astype(BF16)
            return carry

        def norm_part(i, carry):
            pltpu.make_async_copy(x_hbm.at[pl.ds(group * ROWS + i * xr, xr)], x_buf.at[pl.ds(i * xr, xr)], x_sem.at[i]).wait()
            return lax.fori_loop(i * (xr // step), (i + 1) * (xr // step), norm, carry)

        lax.fori_loop(0, nx, norm_part, 0)

        if with_kv:
            kv_loads[0].wait()
            acc = jnp.dot(h_ref[...], ring[0], preferred_element_type=F32)
            for g in range(bn // HEAD):
                cols = slice(g * HEAD, (g + 1) * HEAD)
                kv_ref[:, cols] = rope_head(acc[:, cols], cos_ref[...], sin_ref[...])
            q_load(slots - 2).start()
            kv_loads[1].wait()
            kv_ref[:, kv_cols:] = jnp.dot(h_ref[...], ring[1], preferred_element_type=F32).astype(BF16)
            q_load(slots - 1).start()
            pl.semaphore_wait(barrier, 2)
            sends = []
            for n, (dst, peer) in enumerate(((r2, across), (r1, core))):
                sends.append(pltpu.make_async_remote_copy(src_ref=kv_ref, dst_ref=dst, send_sem=s_sem.at[n], recv_sem=r_sem.at[n], device_id={'cp': peer}, device_id_type=pl.DeviceIdType.MESH))
                sends[-1].start()
            forward = pltpu.make_async_remote_copy(src_ref=r2, dst_ref=r3, send_sem=s_sem.at[2], recv_sem=r_sem.at[2], device_id={'cp': core}, device_id_type=pl.DeviceIdType.MESH)

        def q_store(b):
            cols = pl.ds(pl.multiple_of(b * bn, bn), bn)
            return pltpu.make_async_copy(q_buf.at[:, cols], q_hbm.at[:, cols], q_sem.at[b])

        def q_block(b, carry):
            slot = lax.rem(b + lead, slots)
            q_load(b).wait()
            acc = jnp.dot(h_ref[:ROWS], ring[slot], preferred_element_type=F32)

            @pl.when(b + slots < nq)
            def _():
                q_load(b + slots).start()

            for g in range(bn // HEAD):
                at = pl.ds(pl.multiple_of(b * bn + g * HEAD, HEAD), HEAD)
                q_buf[:, at] = rope_head(acc[:, g * HEAD:(g + 1) * HEAD], cos_ref[:ROWS], sin_ref[:ROWS])
            q_store(b).start()
            if with_kv:
                @pl.when(b == nq - 2)
                def _():
                    sends[0].wait_recv()
                    forward.start()

            return carry

        lax.fori_loop(0, nq, q_block, 0)
        for b in range(nq):
            q_store(b).wait()
        if with_kv:
            sends[0].wait_send()
            sends[1].wait()
            forward.wait()

    whole = lambda arr: pl.BlockSpec(arr.shape, lambda i: (0, 0))
    kv_shape = jax.ShapeDtypeStruct((rows, 2 * kv_cols), BF16)
    kv_out = [kv_shape] * 4 if with_kv else []
    return pl.pallas_call(
        kernel,
        grid=(1,),
        in_specs=[any_spec(), whole(gain), whole(pos2), whole(inv_freq), any_spec()] + [any_spec()] * lead,
        out_specs=[any_spec()] + ([pl.BlockSpec(kv_shape.shape, lambda i: (0, 0)), any_spec(), any_spec(), any_spec()] if with_kv else []),
        out_shape=[jax.ShapeDtypeStruct((ROWS, q_cols), BF16)] + kv_out,
        scratch_shapes=[
            pltpu.VMEM((rows, d_model), BF16),
            pltpu.VMEM((rows, d_model), BF16),
            pltpu.VMEM((slots, d_model, bn), BF16),
            pltpu.VMEM((ROWS, q_cols), BF16),
            pltpu.VMEM((rows, HEAD), F32),
            pltpu.VMEM((rows, HEAD), F32),
            pltpu.VMEM((1, HEAD), F32),
            pltpu.SemaphoreType.DMA((nx,)),
            pltpu.SemaphoreType.DMA((slots,)),
            pltpu.SemaphoreType.DMA((nq,)),
        ] + ([pltpu.SemaphoreType.DMA((3,))] * 2 if with_kv else []),
        compiler_params=pltpu.CompilerParams(vmem_limit_bytes=VMEM_BYTES, collective_id=group, has_side_effects=True) if with_kv else pltpu.CompilerParams(vmem_limit_bytes=VMEM_BYTES),
        cost_estimate=pl.CostEstimate(flops=2 * rows * d_model * (2 * kv_cols + q_cols), bytes_accessed=2 * d_model * (rows + q_cols), transcendentals=0),
        name="front",
    )(x_in, gain, pos2, inv_freq, w_q, *((w_k, w_v) if with_kv else ()))


def attend_send(row_group, cp_size, pos, pos2, q, kv_parts, w_o, cols):
    half = row_group // 2
    qb = kb = ROWS
    rows = 2 * ROWS
    kv_heads = kv_parts[0].shape[1] // (2 * HEAD)
    group = q.shape[1] // (kv_heads * HEAD)
    keys = cp_size * rows * (1 + half)
    scale = HEAD ** -0.5
    parts = len(kv_parts)
    k_dim = q.shape[1]
    half_cols = w_o.shape[1] // 2
    bn = 512

    def kernel(pos_ref, pos2_ref, q_hbm, w_hbm, *rest):
        kv_hbm = rest[:parts]
        o_ref, part_ref, kv_all, q_buf, w_buf, s_ref, p_ref, m_ref, l_ref, acc_ref, kv_sem, q_sem, w_sem = rest[parts:]
        dev, tp = lax.axis_index('cp'), lax.axis_index('tp')
        copies = []
        for n in range(parts):
            owner = lax.bitwise_xor(dev, n % cp_size)
            piece = owner if n < cp_size else 2 * cp_size - 1 - owner
            copies.append(pltpu.make_async_copy(kv_hbm[n], kv_all.at[pl.ds(pl.multiple_of(piece * rows, rows), rows)], kv_sem.at[n]))
            copies[-1].start()

        def q_copy(n):
            at = pl.ds(pl.multiple_of(n * group * HEAD, group * HEAD), group * HEAD)
            return pltpu.make_async_copy(q_hbm.at[:, at], q_buf.at[:, at], q_sem.at[n])

        for n in range(kv_heads):
            q_copy(n).start()

        def w_copy(j):
            at = pl.ds(pl.multiple_of((1 - tp) * half_cols + j * bn, bn), bn)
            return pltpu.make_async_copy(w_hbm.at[:, at], w_buf.at[j], w_sem.at[j])

        for j in range(cols // bn):
            w_copy(j).start()
        for copy in copies:
            copy.wait()
        piece = dev if half == 0 else 2 * cp_size - 1 - dev
        lane = lax.broadcasted_iota(jnp.int32, (qb, LANES), 1)
        t0 = piece * rows + (row_group % 2) * qb
        p0 = pos_ref[row_group * qb]
        t_idx = t0 + lax.broadcasted_iota(jnp.int32, (qb, LANES), 0)
        pos_row = pos2_ref[row_group:row_group + 1, :].astype(F32)
        first = t_idx - jnp.transpose(jnp.broadcast_to(pos_row, (qb, LANES))).astype(jnp.int32)

        def kv_head(n, carry):
            q_copy(n).wait()

            def head_cols(g):
                return pl.ds(pl.multiple_of((n * group + g) * HEAD, HEAD), HEAD)

            k_cols = pl.ds(pl.multiple_of(n * HEAD, HEAD), HEAD)
            v_cols = pl.ds(pl.multiple_of((kv_heads + n) * HEAD, HEAD), HEAD)
            q_stack = jnp.concatenate([q_buf[:, head_cols(g)] for g in range(group)], axis=0)

            @pl.when(p0 <= kb)
            def _():
                w0 = pl.multiple_of(jnp.maximum(t0 - kb, 0), kb)
                at = pl.ds(w0, 2 * kb)
                s_ref[...] = lax.dot_general(q_stack, kv_all[at, k_cols], (((1,), (1,)), ((), ())), preferred_element_type=F32)
                u = w0 + lane
                visible = jnp.concatenate([(u >= first) & (u <= t_idx), (u + kb >= first) & (u + kb <= t_idx)], axis=1)
                for g in range(group):
                    at_g = slice(g * qb, (g + 1) * qb)
                    s = jnp.where(visible, s_ref[at_g] * scale, -1e30)
                    s_ref[at_g] = s
                    m_ref[g] = jnp.broadcast_to(jnp.max(s, axis=1, keepdims=True), (qb, LANES))
                for g in range(group):
                    at_g = slice(g * qb, (g + 1) * qb)
                    m = m_ref[g]
                    e = jnp.exp(s_ref[at_g] - jnp.concatenate([m, m], axis=1))
                    s_ref[at_g] = e
                    l_ref[g] = 1.0 / jnp.broadcast_to(jnp.sum(e, axis=1, keepdims=True), (qb, LANES))
                for g in range(group):
                    at_g = slice(g * qb, (g + 1) * qb)
                    inv = l_ref[g]
                    p_ref[at_g] = (s_ref[at_g] * jnp.concatenate([inv, inv], axis=1)).astype(BF16)
                o = jnp.dot(p_ref[...], kv_all[at, v_cols], preferred_element_type=F32).astype(BF16)
                for g in range(group):
                    o_ref[:, head_cols(g)] = o[g * qb:(g + 1) * qb]

            @pl.when(p0 > kb)
            def _():
                kb0 = lax.div(t0 - p0, kb)
                kb1 = lax.div(t0, kb) + 1
                m_ref[...] = jnp.full_like(m_ref, -1e30)
                l_ref[...] = jnp.zeros_like(l_ref)
                acc_ref[...] = jnp.zeros_like(acc_ref)

                def block(j):
                    at = pl.ds(pl.multiple_of(j * kb, kb), kb)
                    u = j * kb + lane
                    s_ref[:, :kb] = lax.dot_general(q_stack, kv_all[at, k_cols], (((1,), (1,)), ((), ())), preferred_element_type=F32)
                    return at, (u >= first) & (u <= t_idx)

                def head_scores(g, visible):
                    at_g = pl.ds(pl.multiple_of(g * qb, qb), qb)
                    return at_g, jnp.where(visible, s_ref[at_g, :kb] * scale, -1e30)

                def stats(j, carry):
                    _, visible = block(j)

                    def one(g, inner):
                        _, s = head_scores(g, visible)
                        m_old = m_ref[g]
                        m_new = jnp.maximum(m_old, jnp.max(s, axis=1, keepdims=True))
                        l_ref[g] = l_ref[g] * jnp.exp(m_old - m_new) + jnp.sum(jnp.exp(s - m_new), axis=1, keepdims=True)
                        m_ref[g] = m_new
                        return inner

                    return lax.fori_loop(0, group, one, carry)

                def weigh(j, carry):
                    at, visible = block(j)

                    def one(g, inner):
                        at_g, s = head_scores(g, visible)
                        p_ref[at_g, :kb] = (jnp.exp(s - m_ref[g]) / l_ref[g]).astype(BF16)
                        return inner

                    lax.fori_loop(0, group, one, 0)
                    acc_ref[...] += jnp.dot(p_ref[:, :kb], kv_all[at, v_cols], preferred_element_type=F32)
                    return carry

                lax.fori_loop(kb0, kb1, stats, 0)
                lax.fori_loop(kb0, kb1, weigh, 0)
                for g in range(group):
                    o_ref[:, head_cols(g)] = acc_ref[g * qb:(g + 1) * qb].astype(BF16)

            return carry

        lax.fori_loop(0, kv_heads, kv_head, 0)

        def product(j, carry):
            w_copy(j).wait()
            part_ref[:, pl.ds(pl.multiple_of(j * bn, bn), bn)] = jnp.dot(o_ref[...], w_buf[j], preferred_element_type=F32)
            return carry

        lax.fori_loop(0, cols // bn, product, 0)

    whole = lambda shape: pl.BlockSpec(shape, lambda i, *_: (0, 0))
    return pl.pallas_call(
        kernel,
        grid_spec=pltpu.PrefetchScalarGridSpec(
            num_scalar_prefetch=1,
            grid=(1,),
            in_specs=[whole(pos2.shape), any_spec(), any_spec()] + [any_spec()] * parts,
            out_specs=[whole(q.shape), whole((ROWS, cols))],
            scratch_shapes=[
                pltpu.VMEM((keys, kv_parts[0].shape[1]), BF16),
                pltpu.VMEM(q.shape, BF16),
                pltpu.VMEM((cols // bn, k_dim, bn), BF16),
                pltpu.VMEM((group * qb, 2 * kb), F32),
                pltpu.VMEM((group * qb, 2 * kb), BF16),
                pltpu.VMEM((group, qb, LANES), F32),
                pltpu.VMEM((group, qb, LANES), F32),
                pltpu.VMEM((group * qb, HEAD), F32),
                pltpu.SemaphoreType.DMA((parts,)),
                pltpu.SemaphoreType.DMA((kv_heads,)),
                pltpu.SemaphoreType.DMA((cols // bn,)),
            ],
        ),
        out_shape=[jax.ShapeDtypeStruct(q.shape, BF16), jax.ShapeDtypeStruct((ROWS, cols), F32)],
        compiler_params=pltpu.CompilerParams(vmem_limit_bytes=VMEM_BYTES),
        cost_estimate=pl.CostEstimate(flops=4 * ROWS * k_dim * 512 + 2 * ROWS * k_dim * cols, bytes_accessed=2 * k_dim * cols, transcendentals=0),
        name="attend_send",
    )(pos, pos2, q, w_o, *kv_parts)


def out_send(tp_me, o, w_o, col0, cols):
    rows, k_dim = o.shape
    bn = 512
    own_blocks = w_o.shape[1] // 2 // bn

    def kernel(tp_ref, o_ref, w_ref, part_ref):
        part_ref[...] = jnp.dot(o_ref[...], w_ref[...], preferred_element_type=F32)

    return pl.pallas_call(
        kernel,
        grid_spec=pltpu.PrefetchScalarGridSpec(
            num_scalar_prefetch=1,
            grid=(cols // bn,),
            in_specs=[pl.BlockSpec((rows, k_dim), lambda i, tp: (0, 0)), pl.BlockSpec((k_dim, bn), lambda i, tp: (0, (1 - tp[0]) * own_blocks + col0 // bn + i))],
            out_specs=pl.BlockSpec((rows, bn), lambda i, tp: (0, i)),
        ),
        out_shape=jax.ShapeDtypeStruct((rows, cols), F32),
        compiler_params=pltpu.CompilerParams(vmem_limit_bytes=VMEM_BYTES),
        cost_estimate=pl.CostEstimate(flops=2 * rows * k_dim * cols, bytes_accessed=2 * k_dim * (rows + cols), transcendentals=0),
        name="out_send",
    )(tp_me, o, w_o)


def out_own(row_group, tp_me, o, w_o, x_in, recvs, y_buf, col0):
    rows, k_dim = o.shape
    bn = 512
    own_blocks = w_o.shape[1] // 2 // bn
    starts = [sum(r.shape[1] for r in recvs[:n]) // bn for n in range(len(recvs) + 1)]
    cols = starts[-1] * bn

    def col(i, tp):
        return tp[0] * own_blocks + col0 // bn + i

    def kernel(tp_ref, o_ref, w_ref, x_ref, *rest):
        y_ref, c_ref = rest[-2:]
        acc = jnp.dot(o_ref[...], w_ref[...], preferred_element_type=F32)
        step = pl.program_id(0)
        for n in range(len(recvs)):
            @pl.when((step >= starts[n]) & (step < starts[n + 1]))
            def _():
                out = (x_ref[...].astype(F32) + (acc + rest[n][...])).astype(BF16)
                y_ref[...] = out
                c_ref[...] = out

    def recv_spec(n):
        return pl.BlockSpec((rows, bn), lambda i, tp: (0, jnp.clip(i - starts[n], 0, starts[n + 1] - starts[n] - 1)))

    ins = [o, w_o, x_in] + list(recvs) + ([] if y_buf is None else [y_buf])
    wide = pl.BlockSpec((rows, bn), lambda i, tp: (row_group, col(i, tp)))
    narrow = pl.BlockSpec((rows, bn), lambda i, tp: (0, i))
    return pl.pallas_call(
        kernel,
        grid_spec=pltpu.PrefetchScalarGridSpec(
            num_scalar_prefetch=1,
            grid=(cols // bn,),
            in_specs=[pl.BlockSpec((rows, k_dim), lambda i, tp: (0, 0)), pl.BlockSpec((k_dim, bn), lambda i, tp: (0, col(i, tp))), wide] + [recv_spec(n) for n in range(len(recvs))] + ([] if y_buf is None else [any_spec()]),
            out_specs=[wide, narrow],
        ),
        out_shape=[jax.ShapeDtypeStruct(x_in.shape, BF16), jax.ShapeDtypeStruct((rows, cols), BF16)],
        input_output_aliases={} if y_buf is None else {len(ins): 0},
        compiler_params=pltpu.CompilerParams(vmem_limit_bytes=VMEM_BYTES),
        cost_estimate=pl.CostEstimate(flops=2 * rows * k_dim * cols, bytes_accessed=2 * k_dim * (rows + cols), transcendentals=0),
        name="out_own",
    )(tp_me, *ins)


def place(row_group, tp_me, recv, y_buf, col0):
    rows, cols = recv.shape
    bn = 512
    own_blocks = y_buf.shape[1] // 2 // bn

    def kernel(tp_ref, r_ref, y_in, y_ref):
        y_ref[...] = r_ref[...]

    return pl.pallas_call(
        kernel,
        grid_spec=pltpu.PrefetchScalarGridSpec(
            num_scalar_prefetch=1,
            grid=(cols // bn,),
            in_specs=[pl.BlockSpec((rows, bn), lambda i, tp: (0, i)), any_spec()],
            out_specs=pl.BlockSpec((rows, bn), lambda i, tp: (row_group, (1 - tp[0]) * own_blocks + col0 // bn + i)),
        ),
        out_shape=jax.ShapeDtypeStruct(y_buf.shape, BF16),
        input_output_aliases={2: 0},
        cost_estimate=pl.CostEstimate(flops=rows * cols, bytes_accessed=4 * rows * cols, transcendentals=0),
        name="place",
    )(tp_me, recv, y_buf)


def solution(mesh):
    cp_size = mesh.shape['cp']
    tp_size = mesh.shape['tp']
    swap_tp = [(j, tp_size - 1 - j) for j in range(tp_size)]

    def local_step(x_in, doc_id, pos_in_doc, norm_gain, w_q, w_k, w_v, w_o, inv_freq):
        local_rows, d_model = x_in.shape
        kv_cols = w_k.shape[1]
        groups = local_rows // ROWS
        tp_me = lax.axis_index('tp').astype(jnp.int32).reshape(1)
        gain = norm_gain.reshape(1, d_model)
        pos2 = pos_in_doc.reshape(groups, LANES)
        freq = inv_freq.reshape(1, HEAD // 2)
        kv_parts = []
        attn, sent, results = {}, {}, []
        y_buf = None

        def swap(value):
            return lax.ppermute(value, 'tp', swap_tp)

        def make(r):
            q, *parts = front(r, r % 2 == 0, x_in, gain, pos2, freq, w_q, w_k, w_v)
            kv_parts.extend(parts)
            sizes = CHUNKS[r]
            attn[r], part = attend_send(r, cp_size, pos_in_doc, pos2, q, kv_parts, w_o, sizes[0])
            sent[r] = [swap(part)]
            for c in range(1, len(sizes)):
                part = out_send(tp_me, attn[r], w_o, sum(sizes[:c]), sizes[c])
                sent[r].append(swap(part))

        for kind, r, c0, c1 in PLAN:
            if kind == "make":
                make(r)
                continue
            col0 = sum(CHUNKS[r][:c0])
            y_buf, block = out_own(r, tp_me, attn[r], w_o, x_in, sent[r][c0:c1], y_buf, col0)
            results.append((r, col0, swap(block)))
        for r, col0, block in results:
            y_buf = place(r, tp_me, block, y_buf, col0)
        kv_all = jnp.concatenate([kv_parts[0], kv_parts[cp_size]], axis=0)
        k_out = kv_all[:, :kv_cols].reshape(local_rows, kv_cols // HEAD, HEAD)
        v_out = kv_all[:, kv_cols:].reshape(local_rows, kv_cols // HEAD, HEAD)
        return y_buf, k_out, v_out

    row_spec = P(('dp', 'cp'))
    in_specs = (P(('dp', 'cp'), None), row_spec, row_spec, P(), P(None, 'tp'), P(None, 'tp'), P(None, 'tp'), P('tp', None), P())
    out_specs = (P(('dp', 'cp'), None), P(('dp', 'cp'), 'tp', None), P(('dp', 'cp'), 'tp', None))

    return jax.shard_map(local_step, mesh=mesh, in_specs=in_specs, out_specs=out_specs, check_vma=False)
```

```python
import jax
import jax.numpy as jnp
from jax import lax
from jax.experimental import pallas as pl
from jax.experimental.pallas import tpu as pltpu
from jax.sharding import PartitionSpec as P


F32 = jnp.float32
BF16 = jnp.bfloat16
HEAD = 128
LANES = 128
VMEM_BYTES = 60 * 1024 * 1024
ROWS = 128
CHUNKS = ((1024, 3072), (1024, 3072), (1024, 3072), (2048, 1024, 512, 512))
PLAN = (("make", 0, 0, 2), ("make", 1, 0, 2), ("own", 0, 0, 2), ("make", 2, 0, 2), ("own", 1, 0, 2), ("make", 3, 0, 4), ("own", 2, 0, 2), ("own", 3, 0, 1), ("own", 3, 1, 2), ("own", 3, 2, 3), ("own", 3, 3, 4))


def any_spec():
    return pl.BlockSpec(memory_space=pl.ANY)


def rope_head(vec, cos_t, sin_t):
    vec = vec.astype(BF16).astype(F32)
    return (vec * cos_t + pltpu.roll(vec, HEAD // 2, 1) * sin_t).astype(BF16)


def front(group, with_kv, x_in, gain, pos2, inv_freq, w_q, w_k, w_v):
    d_model = x_in.shape[1]
    kv_cols = w_k.shape[1]
    q_cols = w_q.shape[1]
    bn = kv_cols
    nq = q_cols // bn
    slots = 4
    xr = 64
    rows = 2 * ROWS if with_kv else ROWS
    nx = rows // xr
    step = 32
    lead = 2 if with_kv else 0

    def kernel(x_hbm, gain_ref, pos_ref, freq_ref, wq_hbm, *rest):
        if with_kv:
            wk_hbm, wv_hbm, q_hbm, kv_ref, r1, r2, r3 = rest[:7]
            s_sem, r_sem = rest[-2:]
            rest = rest[7:-2]
            me = lax.axis_index('cp')
            core, across = lax.bitwise_xor(me, 1), lax.bitwise_xor(me, 2)
            barrier = pltpu.get_barrier_semaphore()
            for peer in (core, across):
                pl.semaphore_signal(barrier, inc=1, device_id={'cp': peer}, device_id_type=pl.DeviceIdType.MESH)
        else:
            q_hbm = rest[0]
            rest = rest[1:]
        x_buf, h_ref, ring, q_buf, cos_ref, sin_ref, freq2_ref, x_sem, w_sem, q_sem = rest
        x_copies = [pltpu.make_async_copy(x_hbm.at[pl.ds(group * ROWS + i * xr, xr)], x_buf.at[pl.ds(i * xr, xr)], x_sem.at[i]) for i in range(nx)]
        for copy in x_copies:
            copy.start()

        def q_load(b):
            slot = lax.rem(b + lead, slots)
            return pltpu.make_async_copy(wq_hbm.at[:, pl.ds(pl.multiple_of(b * bn, bn), bn)], ring.at[slot], w_sem.at[slot])

        kv_loads = [pltpu.make_async_copy(w_hbm, ring.at[n], w_sem.at[n]) for n, w_hbm in enumerate((wk_hbm, wv_hbm))] if with_kv else []
        for load in kv_loads:
            load.start()
        for b in range(slots - lead):
            q_load(b).start()

        half_dim = HEAD // 2
        freq2_ref[:, :half_dim] = freq_ref[...]
        freq2_ref[:, half_dim:] = freq_ref[...]
        sign = jnp.where(lax.broadcasted_iota(jnp.int32, (LANES, HEAD), 1) < half_dim, -1.0, 1.0)
        for b in range(rows // LANES):
            pos_row = pos_ref[group + b:group + b + 1, :].astype(F32)
            angle = jnp.transpose(jnp.broadcast_to(pos_row, (LANES, LANES))) * freq2_ref[...]
            cos_ref[b * LANES:(b + 1) * LANES, :] = jnp.cos(angle)
            sin_ref[b * LANES:(b + 1) * LANES, :] = jnp.sin(angle) * sign

        def norm(r, carry):
            at = pl.ds(pl.multiple_of(r * step, step), step)
            total = jnp.zeros((step, LANES), F32)
            for c in range(d_model // LANES):
                v = x_buf[at, c * LANES:(c + 1) * LANES].astype(F32)
                total += v * v
            inv = lax.rsqrt(jnp.sum(total, axis=1, keepdims=True) / d_model + 1e-5)
            for c in range(d_model // LANES):
                cols = slice(c * LANES, (c + 1) * LANES)
                h_ref[at, cols] = (x_buf[at, cols].astype(F32) * inv * gain_ref[:, cols]).astype(BF16)
            return carry

        def norm_part(i, carry):
            pltpu.make_async_copy(x_hbm.at[pl.ds(group * ROWS + i * xr, xr)], x_buf.at[pl.ds(i * xr, xr)], x_sem.at[i]).wait()
            return lax.fori_loop(i * (xr // step), (i + 1) * (xr // step), norm, carry)

        lax.fori_loop(0, nx, norm_part, 0)

        if with_kv:
            kv_loads[0].wait()
            acc = jnp.dot(h_ref[...], ring[0], preferred_element_type=F32)
            for g in range(bn // HEAD):
                cols = slice(g * HEAD, (g + 1) * HEAD)
                kv_ref[:, cols] = rope_head(acc[:, cols], cos_ref[...], sin_ref[...])
            q_load(slots - 2).start()
            kv_loads[1].wait()
            kv_ref[:, kv_cols:] = jnp.dot(h_ref[...], ring[1], preferred_element_type=F32).astype(BF16)
            q_load(slots - 1).start()
            pl.semaphore_wait(barrier, 2)
            sends = []
            for n, (dst, peer) in enumerate(((r2, across), (r1, core))):
                sends.append(pltpu.make_async_remote_copy(src_ref=kv_ref, dst_ref=dst, send_sem=s_sem.at[n], recv_sem=r_sem.at[n], device_id={'cp': peer}, device_id_type=pl.DeviceIdType.MESH))
                sends[-1].start()
            forward = pltpu.make_async_remote_copy(src_ref=r2, dst_ref=r3, send_sem=s_sem.at[2], recv_sem=r_sem.at[2], device_id={'cp': core}, device_id_type=pl.DeviceIdType.MESH)

        def q_store(b):
            cols = pl.ds(pl.multiple_of(b * bn, bn), bn)
            return pltpu.make_async_copy(q_buf.at[:, cols], q_hbm.at[:, cols], q_sem.at[b])

        def q_block(b, carry):
            slot = lax.rem(b + lead, slots)
            q_load(b).wait()
            acc = jnp.dot(h_ref[:ROWS], ring[slot], preferred_element_type=F32)

            @pl.when(b + slots < nq)
            def _():
                q_load(b + slots).start()

            for g in range(bn // HEAD):
                at = pl.ds(pl.multiple_of(b * bn + g * HEAD, HEAD), HEAD)
                q_buf[:, at] = rope_head(acc[:, g * HEAD:(g + 1) * HEAD], cos_ref[:ROWS], sin_ref[:ROWS])
            q_store(b).start()
            if with_kv:
                @pl.when(b == nq - 2)
                def _():
                    sends[0].wait_recv()
                    forward.start()

            return carry

        lax.fori_loop(0, nq, q_block, 0)
        for b in range(nq):
            q_store(b).wait()
        if with_kv:
            sends[0].wait_send()
            sends[1].wait()
            forward.wait()

    whole = lambda arr: pl.BlockSpec(arr.shape, lambda i: (0, 0))
    kv_shape = jax.ShapeDtypeStruct((rows, 2 * kv_cols), BF16)
    kv_out = [kv_shape] * 4 if with_kv else []
    return pl.pallas_call(
        kernel,
        grid=(1,),
        in_specs=[any_spec(), whole(gain), whole(pos2), whole(inv_freq), any_spec()] + [any_spec()] * lead,
        out_specs=[any_spec()] + ([pl.BlockSpec(kv_shape.shape, lambda i: (0, 0)), any_spec(), any_spec(), any_spec()] if with_kv else []),
        out_shape=[jax.ShapeDtypeStruct((ROWS, q_cols), BF16)] + kv_out,
        scratch_shapes=[
            pltpu.VMEM((rows, d_model), BF16),
            pltpu.VMEM((rows, d_model), BF16),
            pltpu.VMEM((slots, d_model, bn), BF16),
            pltpu.VMEM((ROWS, q_cols), BF16),
            pltpu.VMEM((rows, HEAD), F32),
            pltpu.VMEM((rows, HEAD), F32),
            pltpu.VMEM((1, HEAD), F32),
            pltpu.SemaphoreType.DMA((nx,)),
            pltpu.SemaphoreType.DMA((slots,)),
            pltpu.SemaphoreType.DMA((nq,)),
        ] + ([pltpu.SemaphoreType.DMA((3,))] * 2 if with_kv else []),
        compiler_params=pltpu.CompilerParams(vmem_limit_bytes=VMEM_BYTES, collective_id=group, has_side_effects=True) if with_kv else pltpu.CompilerParams(vmem_limit_bytes=VMEM_BYTES),
        cost_estimate=pl.CostEstimate(flops=2 * rows * d_model * (2 * kv_cols + q_cols), bytes_accessed=2 * d_model * (rows + q_cols), transcendentals=0),
        name="front",
    )(x_in, gain, pos2, inv_freq, w_q, *((w_k, w_v) if with_kv else ()))


def attend_send(row_group, cp_size, pos, pos2, q, kv_parts, w_o, cols):
    half = row_group // 2
    qb = kb = ROWS
    rows = 2 * ROWS
    kv_heads = kv_parts[0].shape[1] // (2 * HEAD)
    group = q.shape[1] // (kv_heads * HEAD)
    keys = cp_size * rows * (1 + half)
    scale = HEAD ** -0.5
    parts = len(kv_parts)
    k_dim = q.shape[1]
    half_cols = w_o.shape[1] // 2
    bn = 512
    unroll = 2 if row_group == 0 else 1

    def kernel(pos_ref, pos2_ref, q_hbm, w_hbm, *rest):
        kv_hbm = rest[:parts]
        o_hbm, part_hbm, kv_all, q_buf, o_buf, part_buf, w_buf, s_ref, p_ref, m_ref, l_ref, acc_ref, kv_sem, q_sem, w_sem, o_sem, p_sem = rest[parts:]
        dev, tp = lax.axis_index('cp'), lax.axis_index('tp')
        copies = []
        for n in range(parts):
            owner = lax.bitwise_xor(dev, n % cp_size)
            piece = owner if n < cp_size else 2 * cp_size - 1 - owner
            copies.append(pltpu.make_async_copy(kv_hbm[n], kv_all.at[pl.ds(pl.multiple_of(piece * rows, rows), rows)], kv_sem.at[n]))
            copies[-1].start()

        def q_copy(n):
            at = pl.ds(pl.multiple_of(n * group * HEAD, group * HEAD), group * HEAD)
            return pltpu.make_async_copy(q_hbm.at[:, at], q_buf.at[:, at], q_sem.at[n])

        for n in range(kv_heads):
            q_copy(n).start()

        def w_copy(j):
            at = pl.ds(pl.multiple_of((1 - tp) * half_cols + j * bn, bn), bn)
            return pltpu.make_async_copy(w_hbm.at[:, at], w_buf.at[j], w_sem.at[j])

        for j in range(cols // bn):
            w_copy(j).start()
        for copy in copies:
            copy.wait()
        piece = dev if half == 0 else 2 * cp_size - 1 - dev
        lane = lax.broadcasted_iota(jnp.int32, (qb, LANES), 1)
        t0 = piece * rows + (row_group % 2) * qb
        p0 = pos_ref[row_group * qb]
        t_idx = t0 + lax.broadcasted_iota(jnp.int32, (qb, LANES), 0)
        pos_row = pos2_ref[row_group:row_group + 1, :].astype(F32)
        first = t_idx - jnp.transpose(jnp.broadcast_to(pos_row, (qb, LANES))).astype(jnp.int32)

        def head_cols(n, g):
            return pl.ds(pl.multiple_of((n * group + g) * HEAD, HEAD), HEAD)

        def kv_cols(n):
            return pl.ds(pl.multiple_of(n * HEAD, HEAD), HEAD)

        def stack(n):
            return jnp.concatenate([q_buf[:, head_cols(n, g)] for g in range(group)], axis=0)

        @pl.when(p0 <= kb)
        def _():
            w0 = pl.multiple_of(jnp.maximum(t0 - kb, 0), kb)
            at = pl.ds(w0, 2 * kb)
            u = w0 + lane
            visible = jnp.concatenate([(u >= first) & (u <= t_idx), (u + kb >= first) & (u + kb <= t_idx)], axis=1)

            def some_heads(i, carry):
                for j in range(unroll):
                    n = i * unroll + j
                    q_copy(n).wait()
                    s_ref[j] = lax.dot_general(stack(n), kv_all[at, kv_cols(n)], (((1,), (1,)), ((), ())), preferred_element_type=F32)
                for j in range(unroll):
                    for g in range(group):
                        at_g = slice(g * qb, (g + 1) * qb)
                        s = jnp.where(visible, s_ref[j, at_g] * scale, -1e30)
                        s_ref[j, at_g] = s
                        m_ref[g] = jnp.broadcast_to(jnp.max(s, axis=1, keepdims=True), (qb, LANES))
                    for g in range(group):
                        at_g = slice(g * qb, (g + 1) * qb)
                        m = m_ref[g]
                        e = jnp.exp(s_ref[j, at_g] - jnp.concatenate([m, m], axis=1))
                        s_ref[j, at_g] = e
                        l_ref[g] = 1.0 / jnp.broadcast_to(jnp.sum(e, axis=1, keepdims=True), (qb, LANES))
                    for g in range(group):
                        at_g = slice(g * qb, (g + 1) * qb)
                        inv = l_ref[g]
                        p_ref[j, at_g] = (s_ref[j, at_g] * jnp.concatenate([inv, inv], axis=1)).astype(BF16)
                    n = i * unroll + j
                    o = jnp.dot(p_ref[j], kv_all[at, kv_cols(kv_heads + n)], preferred_element_type=F32).astype(BF16)
                    for g in range(group):
                        o_buf[:, head_cols(n, g)] = o[g * qb:(g + 1) * qb]
                return carry

            lax.fori_loop(0, kv_heads // unroll, some_heads, 0)

        @pl.when(p0 > kb)
        def _():
            kb0 = lax.div(t0 - p0, kb)
            kb1 = lax.div(t0, kb) + 1

            def kv_head(n, carry):
                q_copy(n).wait()
                q_stack = stack(n)
                m_ref[...] = jnp.full_like(m_ref, -1e30)
                l_ref[...] = jnp.zeros_like(l_ref)
                acc_ref[...] = jnp.zeros_like(acc_ref)

                def block(j):
                    at = pl.ds(pl.multiple_of(j * kb, kb), kb)
                    u = j * kb + lane
                    s_ref[0, :, :kb] = lax.dot_general(q_stack, kv_all[at, kv_cols(n)], (((1,), (1,)), ((), ())), preferred_element_type=F32)
                    return at, (u >= first) & (u <= t_idx)

                def head_scores(g, visible):
                    at_g = pl.ds(pl.multiple_of(g * qb, qb), qb)
                    return at_g, jnp.where(visible, s_ref[0, at_g, :kb] * scale, -1e30)

                def stats(j, inner):
                    _, visible = block(j)

                    def one(g, c):
                        _, s = head_scores(g, visible)
                        m_old = m_ref[g]
                        m_new = jnp.maximum(m_old, jnp.max(s, axis=1, keepdims=True))
                        l_ref[g] = l_ref[g] * jnp.exp(m_old - m_new) + jnp.sum(jnp.exp(s - m_new), axis=1, keepdims=True)
                        m_ref[g] = m_new
                        return c

                    return lax.fori_loop(0, group, one, inner)

                def weigh(j, inner):
                    at, visible = block(j)

                    def one(g, c):
                        at_g, s = head_scores(g, visible)
                        p_ref[0, at_g, :kb] = (jnp.exp(s - m_ref[g]) / l_ref[g]).astype(BF16)
                        return c

                    lax.fori_loop(0, group, one, 0)
                    acc_ref[...] += jnp.dot(p_ref[0, :, :kb], kv_all[at, kv_cols(kv_heads + n)], preferred_element_type=F32)
                    return inner

                lax.fori_loop(kb0, kb1, stats, 0)
                lax.fori_loop(kb0, kb1, weigh, 0)
                for g in range(group):
                    o_buf[:, head_cols(n, g)] = acc_ref[g * qb:(g + 1) * qb].astype(BF16)
                return carry

            lax.fori_loop(0, kv_heads, kv_head, 0)

        o_copy = pltpu.make_async_copy(o_buf, o_hbm, o_sem)
        o_copy.start()

        def part_copy(j):
            at = pl.ds(pl.multiple_of(j * bn, bn), bn)
            return pltpu.make_async_copy(part_buf.at[:, at], part_hbm.at[:, at], p_sem.at[j])

        def product(j, carry):
            w_copy(j).wait()
            part_buf[:, pl.ds(pl.multiple_of(j * bn, bn), bn)] = jnp.dot(o_buf[...], w_buf[j], preferred_element_type=F32)
            part_copy(j).start()
            return carry

        lax.fori_loop(0, cols // bn, product, 0)
        o_copy.wait()
        for j in range(cols // bn):
            part_copy(j).wait()

    whole = lambda shape: pl.BlockSpec(shape, lambda i, *_: (0, 0))
    return pl.pallas_call(
        kernel,
        grid_spec=pltpu.PrefetchScalarGridSpec(
            num_scalar_prefetch=1,
            grid=(1,),
            in_specs=[whole(pos2.shape), any_spec(), any_spec()] + [any_spec()] * parts,
            out_specs=[any_spec(), any_spec()],
            scratch_shapes=[
                pltpu.VMEM((keys, kv_parts[0].shape[1]), BF16),
                pltpu.VMEM(q.shape, BF16),
                pltpu.VMEM(q.shape, BF16),
                pltpu.VMEM((ROWS, cols), F32),
                pltpu.VMEM((cols // bn, k_dim, bn), BF16),
                pltpu.VMEM((unroll, group * qb, 2 * kb), F32),
                pltpu.VMEM((unroll, group * qb, 2 * kb), BF16),
                pltpu.VMEM((group, qb, LANES), F32),
                pltpu.VMEM((group, qb, LANES), F32),
                pltpu.VMEM((group * qb, HEAD), F32),
                pltpu.SemaphoreType.DMA((parts,)),
                pltpu.SemaphoreType.DMA((kv_heads,)),
                pltpu.SemaphoreType.DMA((cols // bn,)),
                pltpu.SemaphoreType.DMA,
                pltpu.SemaphoreType.DMA((cols // bn,)),
            ],
        ),
        out_shape=[jax.ShapeDtypeStruct(q.shape, BF16), jax.ShapeDtypeStruct((ROWS, cols), F32)],
        compiler_params=pltpu.CompilerParams(vmem_limit_bytes=VMEM_BYTES),
        cost_estimate=pl.CostEstimate(flops=4 * ROWS * k_dim * 512 + 2 * ROWS * k_dim * cols, bytes_accessed=2 * k_dim * cols, transcendentals=0),
        name="attend_send",
    )(pos, pos2, q, w_o, *kv_parts)


def out_cols(row_group, o, w_o, col0, cols, x_in=None, recvs=(), y_buf=None):
    rows, k_dim = o.shape
    bn = 512
    nb = cols // bn
    half_cols = w_o.shape[1] // 2
    own = bool(recvs)
    starts = [sum(r.shape[1] for r in recvs[:n]) for n in range(len(recvs))]

    def kernel(o_hbm, w_hbm, *rest):
        if own:
            x_hbm, recv_hbm = rest[0], rest[1:1 + len(recvs)]
            rest = rest[1 + len(recvs) + (y_buf is not None):]
            y_hbm, c_hbm, o_buf, w_buf, c_buf, o_sem, w_sem, c_sem, x_buf, r_buf, x_sem, r_sem, y_sem = rest
        else:
            c_hbm, o_buf, w_buf, c_buf, o_sem, w_sem, c_sem = rest
        tp = lax.axis_index('tp')
        side = tp if own else 1 - tp
        base = side * half_cols + col0

        def w_copy(j):
            return pltpu.make_async_copy(w_hbm.at[:, pl.ds(pl.multiple_of(base + j * bn, bn), bn)], w_buf.at[j], w_sem.at[j])

        def out_copies(j):
            at = pl.ds(pl.multiple_of(j * bn, bn), bn)
            copies = [pltpu.make_async_copy(c_buf.at[:, at], c_hbm.at[:, at], c_sem.at[j])]
            if own:
                to = y_hbm.at[pl.ds(row_group * ROWS, rows), pl.ds(pl.multiple_of(base + j * bn, bn), bn)]
                copies.append(pltpu.make_async_copy(c_buf.at[:, at], to, y_sem.at[j]))
            return copies

        o_copy = pltpu.make_async_copy(o_hbm, o_buf, o_sem)
        o_copy.start()
        w_copy(0).start()
        extra = []
        if own:
            extra.append(pltpu.make_async_copy(x_hbm.at[pl.ds(row_group * ROWS, rows), pl.ds(pl.multiple_of(base, bn), cols)], x_buf, x_sem))
            for n, recv in enumerate(recv_hbm):
                extra.append(pltpu.make_async_copy(recv, r_buf.at[:, starts[n]:starts[n] + recv.shape[1]], r_sem.at[n]))
            for copy in extra:
                copy.start()
        for j in range(1, nb):
            w_copy(j).start()
        o_copy.wait()
        for copy in extra:
            copy.wait()

        def block(j, carry):
            at = pl.ds(pl.multiple_of(j * bn, bn), bn)
            w_copy(j).wait()
            acc = jnp.dot(o_buf[...], w_buf[j], preferred_element_type=F32)
            if own:
                c_buf[:, at] = (x_buf[:, at].astype(F32) + (acc + r_buf[:, at])).astype(BF16)
            else:
                c_buf[:, at] = acc
            for copy in out_copies(j):
                copy.start()
            return carry

        lax.fori_loop(0, nb, block, 0)

        def finish(j, carry):
            for copy in out_copies(j):
                copy.wait()
            return carry

        lax.fori_loop(0, nb, finish, 0)

    kind = BF16 if own else F32
    chunk = jax.ShapeDtypeStruct((rows, cols), kind)
    ins = [o, w_o] + ([x_in, *recvs] if own else []) + ([] if y_buf is None else [y_buf])
    sems = [pltpu.SemaphoreType.DMA, pltpu.SemaphoreType.DMA((nb,)), pltpu.SemaphoreType.DMA((nb,))]
    scratch = [pltpu.VMEM((rows, k_dim), BF16), pltpu.VMEM((nb, k_dim, bn), BF16), pltpu.VMEM((rows, cols), kind)] + sems
    if own:
        scratch += [pltpu.VMEM((rows, cols), BF16), pltpu.VMEM((rows, cols), F32), pltpu.SemaphoreType.DMA, pltpu.SemaphoreType.DMA((len(recvs),)), pltpu.SemaphoreType.DMA((nb,))]
    return pl.pallas_call(
        kernel,
        grid=(1,),
        in_specs=[any_spec()] * len(ins),
        out_specs=[any_spec()] * (2 if own else 1),
        out_shape=([jax.ShapeDtypeStruct(x_in.shape, BF16)] if own else []) + [chunk],
        scratch_shapes=scratch,
        input_output_aliases={} if y_buf is None else {len(ins) - 1: 0},
        compiler_params=pltpu.CompilerParams(vmem_limit_bytes=VMEM_BYTES),
        cost_estimate=pl.CostEstimate(flops=2 * rows * k_dim * cols, bytes_accessed=2 * k_dim * (rows + cols), transcendentals=0),
        name="out_own" if own else "out_send",
    )(*ins)


def place(row_group, tp_me, recv, y_buf, col0):
    rows, cols = recv.shape
    half_cols = y_buf.shape[1] // 2
    bn = min(cols, 2048)

    def kernel(tp_ref, r_ref, y_in, y_ref):
        y_ref[...] = r_ref[...]

    return pl.pallas_call(
        kernel,
        grid_spec=pltpu.PrefetchScalarGridSpec(
            num_scalar_prefetch=1,
            grid=(cols // bn,),
            in_specs=[pl.BlockSpec((rows, bn), lambda i, tp: (0, i)), any_spec()],
            out_specs=pl.BlockSpec((rows, bn), lambda i, tp: (row_group, ((1 - tp[0]) * half_cols + col0) // bn + i)),
        ),
        out_shape=jax.ShapeDtypeStruct(y_buf.shape, BF16),
        input_output_aliases={2: 0},
        compiler_params=pltpu.CompilerParams(vmem_limit_bytes=8 * 1024 * 1024),
        cost_estimate=pl.CostEstimate(flops=rows * cols, bytes_accessed=4 * rows * cols, transcendentals=0),
        name="place",
    )(tp_me, recv, y_buf)


def solution(mesh):
    cp_size = mesh.shape['cp']
    tp_size = mesh.shape['tp']
    swap_tp = [(j, tp_size - 1 - j) for j in range(tp_size)]

    def local_step(x_in, doc_id, pos_in_doc, norm_gain, w_q, w_k, w_v, w_o, inv_freq):
        local_rows, d_model = x_in.shape
        kv_cols = w_k.shape[1]
        groups = local_rows // ROWS
        tp_me = lax.axis_index('tp').astype(jnp.int32).reshape(1)
        gain = norm_gain.reshape(1, d_model)
        pos2 = pos_in_doc.reshape(groups, LANES)
        freq = inv_freq.reshape(1, HEAD // 2)
        kv_parts = []
        attn, sent, results = {}, {}, []
        y_buf = None

        def swap(value):
            return lax.ppermute(value, 'tp', swap_tp)

        def make(r):
            q, *parts = front(r, r % 2 == 0, x_in, gain, pos2, freq, w_q, w_k, w_v)
            kv_parts.extend(parts)
            sizes = CHUNKS[r]
            attn[r], part = attend_send(r, cp_size, pos_in_doc, pos2, q, kv_parts, w_o, sizes[0])
            sent[r] = [swap(part)]
            for c in range(1, len(sizes)):
                part, = out_cols(r, attn[r], w_o, sum(sizes[:c]), sizes[c])
                sent[r].append(swap(part))

        for kind, r, c0, c1 in PLAN:
            if kind == "make":
                make(r)
                continue
            col0 = sum(CHUNKS[r][:c0])
            y_buf, block = out_cols(r, attn[r], w_o, col0, sum(CHUNKS[r][c0:c1]), x_in, sent[r][c0:c1], y_buf)
            results.append((r, col0, swap(block)))
        for r, col0, block in results:
            y_buf = place(r, tp_me, block, y_buf, col0)
        kv_all = jnp.concatenate([kv_parts[0], kv_parts[cp_size]], axis=0)
        k_out = kv_all[:, :kv_cols].reshape(local_rows, kv_cols // HEAD, HEAD)
        v_out = kv_all[:, kv_cols:].reshape(local_rows, kv_cols // HEAD, HEAD)
        return y_buf, k_out, v_out

    row_spec = P(('dp', 'cp'))
    in_specs = (P(('dp', 'cp'), None), row_spec, row_spec, P(), P(None, 'tp'), P(None, 'tp'), P(None, 'tp'), P('tp', None), P())
    out_specs = (P(('dp', 'cp'), None), P(('dp', 'cp'), 'tp', None), P(('dp', 'cp'), 'tp', None))

    return jax.shard_map(local_step, mesh=mesh, in_specs=in_specs, out_specs=out_specs, check_vma=False)
```

```python
import jax
import jax.numpy as jnp
from jax import lax
from jax.experimental import pallas as pl
from jax.experimental.pallas import tpu as pltpu
from jax.sharding import PartitionSpec as P


F32 = jnp.float32
BF16 = jnp.bfloat16
HEAD = 128
LANES = 128
VMEM_BYTES = 60 * 1024 * 1024
ROWS = 128
CHUNKS = ((1024, 3072), (1024, 3072), (1024, 3072), (2048, 1024, 512, 512))
PLAN = (("make", 0, 0, 2), ("make", 1, 0, 2), ("own", 0, 0, 2), ("make", 2, 0, 2), ("own", 1, 0, 2), ("make", 3, 0, 4), ("own", 2, 0, 2), ("own", 3, 0, 1), ("own", 3, 1, 2), ("own", 3, 2, 3), ("own", 3, 3, 4))


def any_spec():
    return pl.BlockSpec(memory_space=pl.ANY)


def rope_head(vec, cos_t, sin_t):
    vec = vec.astype(BF16).astype(F32)
    return (vec * cos_t + pltpu.roll(vec, HEAD // 2, 1) * sin_t).astype(BF16)


def front(group, with_kv, x_in, gain, pos2, inv_freq, w_q, w_k, w_v):
    d_model = x_in.shape[1]
    kv_cols = w_k.shape[1]
    q_cols = w_q.shape[1]
    bn = kv_cols
    nq = q_cols // bn
    slots = 8
    ahead = 4
    deep = d_model // 2
    xr = 64
    rows = 2 * ROWS if with_kv else ROWS
    nx = rows // xr
    step = 32
    lead = 4 if with_kv else 0

    def kernel(x_hbm, gain_ref, pos_ref, freq_ref, wq_hbm, *rest):
        if with_kv:
            wk_hbm, wv_hbm, q_hbm, kv_ref, r1, r2, r3 = rest[:7]
            s_sem, r_sem = rest[-2:]
            rest = rest[7:-2]
            me = lax.axis_index('cp')
            core, across = lax.bitwise_xor(me, 1), lax.bitwise_xor(me, 2)
            barrier = pltpu.get_barrier_semaphore()
            for peer in (core, across):
                pl.semaphore_signal(barrier, inc=1, device_id={'cp': peer}, device_id_type=pl.DeviceIdType.MESH)
        else:
            q_hbm = rest[0]
            rest = rest[1:]
        x_buf, h_ref, ring, q_buf, cos_ref, sin_ref, freq2_ref, x_sem, w_sem, q_sem = rest
        x_copies = [pltpu.make_async_copy(x_hbm.at[pl.ds(group * ROWS + i * xr, xr)], x_buf.at[pl.ds(i * xr, xr)], x_sem.at[i]) for i in range(nx)]
        for copy in x_copies:
            copy.start()

        def q_load(b, part):
            slot = lax.rem(2 * b + part + lead, slots)
            return pltpu.make_async_copy(wq_hbm.at[pl.ds(part * deep, deep), pl.ds(pl.multiple_of(b * bn, bn), bn)], ring.at[slot], w_sem.at[slot])

        def load(u):
            if u >= lead:
                return q_load((u - lead) // 2, u % 2)
            w_hbm = (wk_hbm, wv_hbm)[u // 2]
            return pltpu.make_async_copy(w_hbm.at[pl.ds((u % 2) * deep, deep)], ring.at[u], w_sem.at[u])

        half_dim = HEAD // 2
        freq2_ref[:, :half_dim] = freq_ref[...]
        freq2_ref[:, half_dim:] = freq_ref[...]
        sign = jnp.where(lax.broadcasted_iota(jnp.int32, (LANES, HEAD), 1) < half_dim, -1.0, 1.0)
        for b in range(rows // LANES):
            pos_row = pos_ref[group + b:group + b + 1, :].astype(F32)
            angle = jnp.transpose(jnp.broadcast_to(pos_row, (LANES, LANES))) * freq2_ref[...]
            cos_ref[b * LANES:(b + 1) * LANES, :] = jnp.cos(angle)
            sin_ref[b * LANES:(b + 1) * LANES, :] = jnp.sin(angle) * sign

        load(0).start()
        load(1).start()

        def norm(r, carry):
            at = pl.ds(pl.multiple_of(r * step, step), step)
            total = jnp.zeros((step, LANES), F32)
            for c in range(d_model // LANES):
                v = x_buf[at, c * LANES:(c + 1) * LANES].astype(F32)
                total += v * v
            inv = lax.rsqrt(jnp.sum(total, axis=1, keepdims=True) / d_model + 1e-5)
            for c in range(d_model // LANES):
                cols = slice(c * LANES, (c + 1) * LANES)
                h_ref[at, cols] = (x_buf[at, cols].astype(F32) * inv * gain_ref[:, cols]).astype(BF16)
            return carry

        for i in range(nx):
            x_copies[i].wait()
        load(2).start()
        load(3).start()
        lax.fori_loop(0, rows // step, norm, 0)

        def product(lhs_rows, slots_of, waits, after):
            acc = None
            for part in range(2):
                waits(part)
                after(part)
                half_acc = jnp.dot(h_ref[:lhs_rows, part * deep:(part + 1) * deep], ring[slots_of(part)], preferred_element_type=F32)
                acc = half_acc if acc is None else acc + half_acc
            return acc

        if with_kv:
            for n in range(2):
                acc = product(rows, lambda part: 2 * n + part, lambda part: load(2 * n + part).wait(), lambda part: load(2 * n + part + ahead).start())
                for g in range(bn // HEAD):
                    cols = slice(g * HEAD, (g + 1) * HEAD)
                    to = slice(n * kv_cols + g * HEAD, n * kv_cols + (g + 1) * HEAD)
                    kv_ref[:, to] = rope_head(acc[:, cols], cos_ref[...], sin_ref[...]) if n == 0 else acc[:, cols].astype(BF16)
            pl.semaphore_wait(barrier, 2)
            sends = []
            for n, (dst, peer) in enumerate(((r2, across), (r1, core))):
                sends.append(pltpu.make_async_remote_copy(src_ref=kv_ref, dst_ref=dst, send_sem=s_sem.at[n], recv_sem=r_sem.at[n], device_id={'cp': peer}, device_id_type=pl.DeviceIdType.MESH))
                sends[-1].start()
            forward = pltpu.make_async_remote_copy(src_ref=r2, dst_ref=r3, send_sem=s_sem.at[2], recv_sem=r_sem.at[2], device_id={'cp': core}, device_id_type=pl.DeviceIdType.MESH)

        def q_store(b):
            cols = pl.ds(pl.multiple_of(b * bn, bn), bn)
            return pltpu.make_async_copy(q_buf.at[:, cols], q_hbm.at[:, cols], q_sem.at[b])

        def q_block(b, carry):
            def after(part):
                @pl.when(b + ahead // 2 < nq)
                def _():
                    q_load(b + ahead // 2, part).start()

            acc = product(ROWS, lambda part: lax.rem(2 * b + part + lead, slots), lambda part: q_load(b, part).wait(), after)
            for g in range(bn // HEAD):
                at = pl.ds(pl.multiple_of(b * bn + g * HEAD, HEAD), HEAD)
                q_buf[:, at] = rope_head(acc[:, g * HEAD:(g + 1) * HEAD], cos_ref[:ROWS], sin_ref[:ROWS])
            q_store(b).start()
            if with_kv:
                @pl.when(b == nq - 2)
                def _():
                    sends[0].wait_recv()
                    forward.start()

            return carry

        lax.fori_loop(0, nq, q_block, 0)
        for b in range(nq):
            q_store(b).wait()
        if with_kv:
            sends[0].wait_send()
            sends[1].wait()
            forward.wait()

    whole = lambda arr: pl.BlockSpec(arr.shape, lambda i: (0, 0))
    kv_shape = jax.ShapeDtypeStruct((rows, 2 * kv_cols), BF16)
    kv_out = [kv_shape] * 4 if with_kv else []
    return pl.pallas_call(
        kernel,
        grid=(1,),
        in_specs=[any_spec(), whole(gain), whole(pos2), whole(inv_freq), any_spec()] + [any_spec()] * (2 if with_kv else 0),
        out_specs=[any_spec()] + ([pl.BlockSpec(kv_shape.shape, lambda i: (0, 0)), any_spec(), any_spec(), any_spec()] if with_kv else []),
        out_shape=[jax.ShapeDtypeStruct((ROWS, q_cols), BF16)] + kv_out,
        scratch_shapes=[
            pltpu.VMEM((rows, d_model), BF16),
            pltpu.VMEM((rows, d_model), BF16),
            pltpu.VMEM((slots, deep, bn), BF16),
            pltpu.VMEM((ROWS, q_cols), BF16),
            pltpu.VMEM((rows, HEAD), F32),
            pltpu.VMEM((rows, HEAD), F32),
            pltpu.VMEM((1, HEAD), F32),
            pltpu.SemaphoreType.DMA((nx,)),
            pltpu.SemaphoreType.DMA((slots,)),
            pltpu.SemaphoreType.DMA((nq,)),
        ] + ([pltpu.SemaphoreType.DMA((3,))] * 2 if with_kv else []),
        compiler_params=pltpu.CompilerParams(vmem_limit_bytes=VMEM_BYTES, collective_id=group, has_side_effects=True) if with_kv else pltpu.CompilerParams(vmem_limit_bytes=VMEM_BYTES),
        cost_estimate=pl.CostEstimate(flops=2 * rows * d_model * (2 * kv_cols + q_cols), bytes_accessed=2 * d_model * (rows + q_cols), transcendentals=0),
        name="front",
    )(x_in, gain, pos2, inv_freq, w_q, *((w_k, w_v) if with_kv else ()))


def attend_send(row_group, cp_size, pos, pos2, q, kv_parts, w_o, cols):
    half = row_group // 2
    qb = kb = ROWS
    rows = 2 * ROWS
    kv_heads = kv_parts[0].shape[1] // (2 * HEAD)
    group = q.shape[1] // (kv_heads * HEAD)
    keys = cp_size * rows * (1 + half)
    scale = HEAD ** -0.5
    parts = len(kv_parts)
    k_dim = q.shape[1]
    half_cols = w_o.shape[1] // 2
    bn = 512
    unroll = 2 if row_group == 0 else 1

    def kernel(pos_ref, pos2_ref, q_hbm, w_hbm, *rest):
        kv_hbm = rest[:parts]
        o_hbm, part_hbm, kv_all, q_buf, o_buf, part_buf, w_buf, s_ref, p_ref, m_ref, l_ref, acc_ref, kv_sem, q_sem, w_sem, o_sem, p_sem = rest[parts:]
        dev, tp = lax.axis_index('cp'), lax.axis_index('tp')
        copies = []
        for n in range(parts):
            owner = lax.bitwise_xor(dev, n % cp_size)
            piece = owner if n < cp_size else 2 * cp_size - 1 - owner
            copies.append(pltpu.make_async_copy(kv_hbm[n], kv_all.at[pl.ds(pl.multiple_of(piece * rows, rows), rows)], kv_sem.at[n]))
            copies[-1].start()

        def q_copy(n):
            at = pl.ds(pl.multiple_of(n * group * HEAD, group * HEAD), group * HEAD)
            return pltpu.make_async_copy(q_hbm.at[:, at], q_buf.at[:, at], q_sem.at[n])

        for n in range(kv_heads):
            q_copy(n).start()

        def w_copy(j):
            at = pl.ds(pl.multiple_of((1 - tp) * half_cols + j * bn, bn), bn)
            return pltpu.make_async_copy(w_hbm.at[:, at], w_buf.at[j], w_sem.at[j])

        for copy in copies:
            copy.wait()
        for j in range(cols // bn):
            w_copy(j).start()
        piece = dev if half == 0 else 2 * cp_size - 1 - dev
        lane = lax.broadcasted_iota(jnp.int32, (qb, LANES), 1)
        t0 = piece * rows + (row_group % 2) * qb
        p0 = pos_ref[row_group * qb]
        t_idx = t0 + lax.broadcasted_iota(jnp.int32, (qb, LANES), 0)
        pos_row = pos2_ref[row_group:row_group + 1, :].astype(F32)
        first = t_idx - jnp.transpose(jnp.broadcast_to(pos_row, (qb, LANES))).astype(jnp.int32)

        def head_cols(n, g):
            return pl.ds(pl.multiple_of((n * group + g) * HEAD, HEAD), HEAD)

        def kv_cols(n):
            return pl.ds(pl.multiple_of(n * HEAD, HEAD), HEAD)

        def stack(n):
            return jnp.concatenate([q_buf[:, head_cols(n, g)] for g in range(group)], axis=0)

        @pl.when(p0 <= kb)
        def _():
            w0 = pl.multiple_of(jnp.maximum(t0 - kb, 0), kb)
            at = pl.ds(w0, 2 * kb)
            u = w0 + lane
            visible = jnp.concatenate([(u >= first) & (u <= t_idx), (u + kb >= first) & (u + kb <= t_idx)], axis=1)

            def some_heads(i, carry):
                for j in range(unroll):
                    n = i * unroll + j
                    q_copy(n).wait()
                    s_ref[j] = lax.dot_general(stack(n), kv_all[at, kv_cols(n)], (((1,), (1,)), ((), ())), preferred_element_type=F32)
                for j in range(unroll):
                    for g in range(group):
                        at_g = slice(g * qb, (g + 1) * qb)
                        s = jnp.where(visible, s_ref[j, at_g] * scale, -1e30)
                        s_ref[j, at_g] = s
                        m_ref[g] = jnp.broadcast_to(jnp.max(s, axis=1, keepdims=True), (qb, LANES))
                    for g in range(group):
                        at_g = slice(g * qb, (g + 1) * qb)
                        m = m_ref[g]
                        e = jnp.exp(s_ref[j, at_g] - jnp.concatenate([m, m], axis=1))
                        s_ref[j, at_g] = e
                        l_ref[g] = 1.0 / jnp.broadcast_to(jnp.sum(e, axis=1, keepdims=True), (qb, LANES))
                    for g in range(group):
                        at_g = slice(g * qb, (g + 1) * qb)
                        inv = l_ref[g]
                        p_ref[j, at_g] = (s_ref[j, at_g] * jnp.concatenate([inv, inv], axis=1)).astype(BF16)
                    n = i * unroll + j
                    o = jnp.dot(p_ref[j], kv_all[at, kv_cols(kv_heads + n)], preferred_element_type=F32).astype(BF16)
                    for g in range(group):
                        o_buf[:, head_cols(n, g)] = o[g * qb:(g + 1) * qb]
                return carry

            lax.fori_loop(0, kv_heads // unroll, some_heads, 0)

        @pl.when(p0 > kb)
        def _():
            kb0 = lax.div(t0 - p0, kb)
            kb1 = lax.div(t0, kb) + 1

            def kv_head(n, carry):
                q_copy(n).wait()
                q_stack = stack(n)
                m_ref[...] = jnp.full_like(m_ref, -1e30)
                l_ref[...] = jnp.zeros_like(l_ref)
                acc_ref[...] = jnp.zeros_like(acc_ref)

                def block(j):
                    at = pl.ds(pl.multiple_of(j * kb, kb), kb)
                    u = j * kb + lane
                    s_ref[0, :, :kb] = lax.dot_general(q_stack, kv_all[at, kv_cols(n)], (((1,), (1,)), ((), ())), preferred_element_type=F32)
                    return at, (u >= first) & (u <= t_idx)

                def head_scores(g, visible):
                    at_g = pl.ds(pl.multiple_of(g * qb, qb), qb)
                    return at_g, jnp.where(visible, s_ref[0, at_g, :kb] * scale, -1e30)

                def stats(j, inner):
                    _, visible = block(j)

                    def one(g, c):
                        _, s = head_scores(g, visible)
                        m_old = m_ref[g]
                        m_new = jnp.maximum(m_old, jnp.max(s, axis=1, keepdims=True))
                        l_ref[g] = l_ref[g] * jnp.exp(m_old - m_new) + jnp.sum(jnp.exp(s - m_new), axis=1, keepdims=True)
                        m_ref[g] = m_new
                        return c

                    return lax.fori_loop(0, group, one, inner)

                def weigh(j, inner):
                    at, visible = block(j)

                    def one(g, c):
                        at_g, s = head_scores(g, visible)
                        p_ref[0, at_g, :kb] = (jnp.exp(s - m_ref[g]) / l_ref[g]).astype(BF16)
                        return c

                    lax.fori_loop(0, group, one, 0)
                    acc_ref[...] += jnp.dot(p_ref[0, :, :kb], kv_all[at, kv_cols(kv_heads + n)], preferred_element_type=F32)
                    return inner

                lax.fori_loop(kb0, kb1, stats, 0)
                lax.fori_loop(kb0, kb1, weigh, 0)
                for g in range(group):
                    o_buf[:, head_cols(n, g)] = acc_ref[g * qb:(g + 1) * qb].astype(BF16)
                return carry

            lax.fori_loop(0, kv_heads, kv_head, 0)

        o_copy = pltpu.make_async_copy(o_buf, o_hbm, o_sem)
        o_copy.start()

        def part_copy(j):
            at = pl.ds(pl.multiple_of(j * bn, bn), bn)
            return pltpu.make_async_copy(part_buf.at[:, at], part_hbm.at[:, at], p_sem.at[j])

        def product(j, carry):
            w_copy(j).wait()
            part_buf[:, pl.ds(pl.multiple_of(j * bn, bn), bn)] = jnp.dot(o_buf[...], w_buf[j], preferred_element_type=F32)
            part_copy(j).start()
            return carry

        lax.fori_loop(0, cols // bn, product, 0)
        o_copy.wait()
        for j in range(cols // bn):
            part_copy(j).wait()

    whole = lambda shape: pl.BlockSpec(shape, lambda i, *_: (0, 0))
    return pl.pallas_call(
        kernel,
        grid_spec=pltpu.PrefetchScalarGridSpec(
            num_scalar_prefetch=1,
            grid=(1,),
            in_specs=[whole(pos2.shape), any_spec(), any_spec()] + [any_spec()] * parts,
            out_specs=[any_spec(), any_spec()],
            scratch_shapes=[
                pltpu.VMEM((keys, kv_parts[0].shape[1]), BF16),
                pltpu.VMEM(q.shape, BF16),
                pltpu.VMEM(q.shape, BF16),
                pltpu.VMEM((ROWS, cols), F32),
                pltpu.VMEM((cols // bn, k_dim, bn), BF16),
                pltpu.VMEM((unroll, group * qb, 2 * kb), F32),
                pltpu.VMEM((unroll, group * qb, 2 * kb), BF16),
                pltpu.VMEM((group, qb, LANES), F32),
                pltpu.VMEM((group, qb, LANES), F32),
                pltpu.VMEM((group * qb, HEAD), F32),
                pltpu.SemaphoreType.DMA((parts,)),
                pltpu.SemaphoreType.DMA((kv_heads,)),
                pltpu.SemaphoreType.DMA((cols // bn,)),
                pltpu.SemaphoreType.DMA,
                pltpu.SemaphoreType.DMA((cols // bn,)),
            ],
        ),
        out_shape=[jax.ShapeDtypeStruct(q.shape, BF16), jax.ShapeDtypeStruct((ROWS, cols), F32)],
        compiler_params=pltpu.CompilerParams(vmem_limit_bytes=VMEM_BYTES),
        cost_estimate=pl.CostEstimate(flops=4 * ROWS * k_dim * 512 + 2 * ROWS * k_dim * cols, bytes_accessed=2 * k_dim * cols, transcendentals=0),
        name="attend_send",
    )(pos, pos2, q, w_o, *kv_parts)


def out_cols(row_group, o, w_o, col0, cols, x_in=None, recvs=(), y_buf=None):
    rows, k_dim = o.shape
    bn = 512
    nb = cols // bn
    half_cols = w_o.shape[1] // 2
    own = bool(recvs)
    starts = [sum(r.shape[1] for r in recvs[:n]) for n in range(len(recvs))]

    def kernel(o_hbm, w_hbm, *rest):
        if own:
            x_hbm, recv_hbm = rest[0], rest[1:1 + len(recvs)]
            rest = rest[1 + len(recvs) + (y_buf is not None):]
            y_hbm, c_hbm, o_buf, w_buf, c_buf, o_sem, w_sem, c_sem, x_buf, r_buf, x_sem, r_sem, y_sem = rest
        else:
            c_hbm, o_buf, w_buf, c_buf, o_sem, w_sem, c_sem = rest
        tp = lax.axis_index('tp')
        side = tp if own else 1 - tp
        base = side * half_cols + col0

        def w_copy(j):
            return pltpu.make_async_copy(w_hbm.at[:, pl.ds(pl.multiple_of(base + j * bn, bn), bn)], w_buf.at[j], w_sem.at[j])

        def out_copies(j):
            at = pl.ds(pl.multiple_of(j * bn, bn), bn)
            copies = [pltpu.make_async_copy(c_buf.at[:, at], c_hbm.at[:, at], c_sem.at[j])]
            if own:
                to = y_hbm.at[pl.ds(row_group * ROWS, rows), pl.ds(pl.multiple_of(base + j * bn, bn), bn)]
                copies.append(pltpu.make_async_copy(c_buf.at[:, at], to, y_sem.at[j]))
            return copies

        o_copy = pltpu.make_async_copy(o_hbm, o_buf, o_sem)
        o_copy.start()
        w_copy(0).start()
        extra = []
        if own:
            extra.append(pltpu.make_async_copy(x_hbm.at[pl.ds(row_group * ROWS, rows), pl.ds(pl.multiple_of(base, bn), cols)], x_buf, x_sem))
            for n, recv in enumerate(recv_hbm):
                extra.append(pltpu.make_async_copy(recv, r_buf.at[:, starts[n]:starts[n] + recv.shape[1]], r_sem.at[n]))
            for copy in extra:
                copy.start()
        if nb > 1:
            w_copy(1).start()
        o_copy.wait()
        for copy in extra:
            copy.wait()

        def block(j, carry):
            at = pl.ds(pl.multiple_of(j * bn, bn), bn)
            w_copy(j).wait()

            @pl.when(j + 2 < nb)
            def _():
                w_copy(j + 2).start()

            acc = jnp.dot(o_buf[...], w_buf[j], preferred_element_type=F32)
            if own:
                c_buf[:, at] = (x_buf[:, at].astype(F32) + (acc + r_buf[:, at])).astype(BF16)
            else:
                c_buf[:, at] = acc
            for copy in out_copies(j):
                copy.start()
            return carry

        lax.fori_loop(0, nb, block, 0)

        def finish(j, carry):
            for copy in out_copies(j):
                copy.wait()
            return carry

        lax.fori_loop(0, nb, finish, 0)

    kind = BF16 if own else F32
    chunk = jax.ShapeDtypeStruct((rows, cols), kind)
    ins = [o, w_o] + ([x_in, *recvs] if own else []) + ([] if y_buf is None else [y_buf])
    sems = [pltpu.SemaphoreType.DMA, pltpu.SemaphoreType.DMA((nb,)), pltpu.SemaphoreType.DMA((nb,))]
    scratch = [pltpu.VMEM((rows, k_dim), BF16), pltpu.VMEM((nb, k_dim, bn), BF16), pltpu.VMEM((rows, cols), kind)] + sems
    if own:
        scratch += [pltpu.VMEM((rows, cols), BF16), pltpu.VMEM((rows, cols), F32), pltpu.SemaphoreType.DMA, pltpu.SemaphoreType.DMA((len(recvs),)), pltpu.SemaphoreType.DMA((nb,))]
    return pl.pallas_call(
        kernel,
        grid=(1,),
        in_specs=[any_spec()] * len(ins),
        out_specs=[any_spec()] * (2 if own else 1),
        out_shape=([jax.ShapeDtypeStruct(x_in.shape, BF16)] if own else []) + [chunk],
        scratch_shapes=scratch,
        input_output_aliases={} if y_buf is None else {len(ins) - 1: 0},
        compiler_params=pltpu.CompilerParams(vmem_limit_bytes=VMEM_BYTES),
        cost_estimate=pl.CostEstimate(flops=2 * rows * k_dim * cols, bytes_accessed=2 * k_dim * (rows + cols), transcendentals=0),
        name="out_own" if own else "out_send",
    )(*ins)


def place(row_group, tp_me, recv, y_buf, col0):
    rows, cols = recv.shape
    half_cols = y_buf.shape[1] // 2
    bn = min(cols, 2048)

    def kernel(tp_ref, r_ref, y_in, y_ref):
        y_ref[...] = r_ref[...]

    return pl.pallas_call(
        kernel,
        grid_spec=pltpu.PrefetchScalarGridSpec(
            num_scalar_prefetch=1,
            grid=(cols // bn,),
            in_specs=[pl.BlockSpec((rows, bn), lambda i, tp: (0, i)), any_spec()],
            out_specs=pl.BlockSpec((rows, bn), lambda i, tp: (row_group, ((1 - tp[0]) * half_cols + col0) // bn + i)),
        ),
        out_shape=jax.ShapeDtypeStruct(y_buf.shape, BF16),
        input_output_aliases={2: 0},
        compiler_params=pltpu.CompilerParams(vmem_limit_bytes=8 * 1024 * 1024),
        cost_estimate=pl.CostEstimate(flops=rows * cols, bytes_accessed=4 * rows * cols, transcendentals=0),
        name="place",
    )(tp_me, recv, y_buf)


def solution(mesh):
    cp_size = mesh.shape['cp']
    tp_size = mesh.shape['tp']
    swap_tp = [(j, tp_size - 1 - j) for j in range(tp_size)]

    def local_step(x_in, doc_id, pos_in_doc, norm_gain, w_q, w_k, w_v, w_o, inv_freq):
        local_rows, d_model = x_in.shape
        kv_cols = w_k.shape[1]
        groups = local_rows // ROWS
        tp_me = lax.axis_index('tp').astype(jnp.int32).reshape(1)
        gain = norm_gain.reshape(1, d_model)
        pos2 = pos_in_doc.reshape(groups, LANES)
        freq = inv_freq.reshape(1, HEAD // 2)
        kv_parts = []
        attn, sent, results = {}, {}, []
        y_buf = None

        def swap(value):
            return lax.ppermute(value, 'tp', swap_tp)

        def make(r):
            q, *parts = front(r, r % 2 == 0, x_in, gain, pos2, freq, w_q, w_k, w_v)
            kv_parts.extend(parts)
            sizes = CHUNKS[r]
            attn[r], part = attend_send(r, cp_size, pos_in_doc, pos2, q, kv_parts, w_o, sizes[0])
            sent[r] = [swap(part)]
            for c in range(1, len(sizes)):
                part, = out_cols(r, attn[r], w_o, sum(sizes[:c]), sizes[c])
                sent[r].append(swap(part))

        for kind, r, c0, c1 in PLAN:
            if kind == "make":
                make(r)
                continue
            col0 = sum(CHUNKS[r][:c0])
            y_buf, block = out_cols(r, attn[r], w_o, col0, sum(CHUNKS[r][c0:c1]), x_in, sent[r][c0:c1], y_buf)
            results.append((r, col0, swap(block)))
        for r, col0, block in results:
            y_buf = place(r, tp_me, block, y_buf, col0)
        kv_all = jnp.concatenate([kv_parts[0], kv_parts[cp_size]], axis=0)
        k_out = kv_all[:, :kv_cols].reshape(local_rows, kv_cols // HEAD, HEAD)
        v_out = kv_all[:, kv_cols:].reshape(local_rows, kv_cols // HEAD, HEAD)
        return y_buf, k_out, v_out

    row_spec = P(('dp', 'cp'))
    in_specs = (P(('dp', 'cp'), None), row_spec, row_spec, P(), P(None, 'tp'), P(None, 'tp'), P(None, 'tp'), P('tp', None), P())
    out_specs = (P(('dp', 'cp'), None), P(('dp', 'cp'), 'tp', None), P(('dp', 'cp'), 'tp', None))

    return jax.shard_map(local_step, mesh=mesh, in_specs=in_specs, out_specs=out_specs, check_vma=False)
```

```python
import jax
import jax.numpy as jnp
from jax import lax
from jax.experimental import pallas as pl
from jax.experimental.pallas import tpu as pltpu
from jax.sharding import PartitionSpec as P


F32 = jnp.float32
BF16 = jnp.bfloat16
HEAD = 128
LANES = 128
VMEM_BYTES = 67043328
ROWS = 128
CHUNKS = ((1024, 3072), (1024, 3072), (1024, 3072), (2048, 1024, 512, 512))
PLAN = (("make", 0, 0, 2), ("make", 1, 0, 2), ("own", 0, 0, 2), ("make", 2, 0, 2), ("own", 1, 0, 2), ("make", 3, 0, 4), ("own", 2, 0, 2), ("own", 3, 0, 1), ("own", 3, 1, 2), ("own", 3, 2, 3), ("own", 3, 3, 4))


def any_spec():
    return pl.BlockSpec(memory_space=pl.ANY)


def rope_head(vec, cos_t, sin_t):
    vec = vec.astype(BF16).astype(F32)
    return (vec * cos_t + pltpu.roll(vec, HEAD // 2, 1) * sin_t).astype(BF16)


def front(group, with_kv, x_in, gain, pos2, inv_freq, w_q, w_k, w_v):
    d_model = x_in.shape[1]
    kv_cols = w_k.shape[1]
    q_cols = w_q.shape[1]
    bn = kv_cols
    nq = q_cols // bn
    slots = 8
    ahead = 4
    deep = d_model // 2
    xr = 64
    rows = 2 * ROWS if with_kv else ROWS
    nx = rows // xr
    step = 32
    lead = 4 if with_kv else 0

    def kernel(x_hbm, gain_ref, pos_ref, freq_ref, wq_hbm, *rest):
        if with_kv:
            wk_hbm, wv_hbm, q_hbm, kv_ref, r1, r2, r3 = rest[:7]
            s_sem, r_sem = rest[-2:]
            rest = rest[7:-2]
            me = lax.axis_index('cp')
            core, across = lax.bitwise_xor(me, 1), lax.bitwise_xor(me, 2)
            barrier = pltpu.get_barrier_semaphore()
            for peer in (core, across):
                pl.semaphore_signal(barrier, inc=1, device_id={'cp': peer}, device_id_type=pl.DeviceIdType.MESH)
        else:
            q_hbm = rest[0]
            rest = rest[1:]
        x_buf, h_ref, ring, q_buf, cos_ref, sin_ref, freq2_ref, x_sem, w_sem, q_sem = rest
        x_copies = [pltpu.make_async_copy(x_hbm.at[pl.ds(group * ROWS + i * xr, xr)], x_buf.at[pl.ds(i * xr, xr)], x_sem.at[i]) for i in range(nx)]
        for copy in x_copies:
            copy.start()

        def q_load(b, part):
            slot = lax.rem(2 * b + part + lead, slots)
            return pltpu.make_async_copy(wq_hbm.at[pl.ds(part * deep, deep), pl.ds(pl.multiple_of(b * bn, bn), bn)], ring.at[slot], w_sem.at[slot])

        def load(u):
            if u >= lead:
                return q_load((u - lead) // 2, u % 2)
            w_hbm = (wk_hbm, wv_hbm)[u // 2]
            return pltpu.make_async_copy(w_hbm.at[pl.ds((u % 2) * deep, deep)], ring.at[u], w_sem.at[u])

        load(0).start()
        load(1).start()

        half_dim = HEAD // 2
        freq2_ref[:, :half_dim] = freq_ref[...]
        freq2_ref[:, half_dim:] = freq_ref[...]
        sign = jnp.where(lax.broadcasted_iota(jnp.int32, (LANES, HEAD), 1) < half_dim, -1.0, 1.0)
        for b in range(rows // LANES):
            pos_row = pos_ref[group + b:group + b + 1, :].astype(F32)
            angle = jnp.transpose(jnp.broadcast_to(pos_row, (LANES, LANES))) * freq2_ref[...]
            cos_ref[b * LANES:(b + 1) * LANES, :] = jnp.cos(angle)
            sin_ref[b * LANES:(b + 1) * LANES, :] = jnp.sin(angle) * sign

        def norm(r, carry):
            at = pl.ds(pl.multiple_of(r * step, step), step)
            total = jnp.zeros((step, LANES), F32)
            for c in range(d_model // LANES):
                v = x_buf[at, c * LANES:(c + 1) * LANES].astype(F32)
                total += v * v
            inv = lax.rsqrt(jnp.sum(total, axis=1, keepdims=True) / d_model + 1e-5)
            for c in range(d_model // LANES):
                cols = slice(c * LANES, (c + 1) * LANES)
                h_ref[at, cols] = (x_buf[at, cols].astype(F32) * inv * gain_ref[:, cols]).astype(BF16)
            return carry

        for i in range(nx):
            x_copies[i].wait()
        load(2).start()
        load(3).start()
        lax.fori_loop(0, rows // step, norm, 0)

        def product(lhs_rows, slots_of, waits, after):
            acc = None
            for part in range(2):
                waits(part)
                after(part)
                half_acc = jnp.dot(h_ref[:lhs_rows, part * deep:(part + 1) * deep], ring[slots_of(part)], preferred_element_type=F32)
                acc = half_acc if acc is None else acc + half_acc
            return acc

        if with_kv:
            for n in range(2):
                acc = product(rows, lambda part: 2 * n + part, lambda part: load(2 * n + part).wait(), lambda part: load(2 * n + part + ahead).start())
                for g in range(bn // HEAD):
                    cols = slice(g * HEAD, (g + 1) * HEAD)
                    to = slice(n * kv_cols + g * HEAD, n * kv_cols + (g + 1) * HEAD)
                    kv_ref[:, to] = rope_head(acc[:, cols], cos_ref[...], sin_ref[...]) if n == 0 else acc[:, cols].astype(BF16)
            pl.semaphore_wait(barrier, 2)
            sends = []
            for n, (dst, peer) in enumerate(((r2, across), (r1, core))):
                sends.append(pltpu.make_async_remote_copy(src_ref=kv_ref, dst_ref=dst, send_sem=s_sem.at[n], recv_sem=r_sem.at[n], device_id={'cp': peer}, device_id_type=pl.DeviceIdType.MESH))
                sends[-1].start()
            forward = pltpu.make_async_remote_copy(src_ref=r2, dst_ref=r3, send_sem=s_sem.at[2], recv_sem=r_sem.at[2], device_id={'cp': core}, device_id_type=pl.DeviceIdType.MESH)

        def q_store(b):
            cols = pl.ds(pl.multiple_of(b * bn, bn), bn)
            return pltpu.make_async_copy(q_buf.at[:, cols], q_hbm.at[:, cols], q_sem.at[b])

        def q_block(b, carry):
            def after(part):
                @pl.when(b + ahead // 2 < nq)
                def _():
                    q_load(b + ahead // 2, part).start()

            acc = product(ROWS, lambda part: lax.rem(2 * b + part + lead, slots), lambda part: q_load(b, part).wait(), after)
            for g in range(bn // HEAD):
                at = pl.ds(pl.multiple_of(b * bn + g * HEAD, HEAD), HEAD)
                q_buf[:, at] = rope_head(acc[:, g * HEAD:(g + 1) * HEAD], cos_ref[:ROWS], sin_ref[:ROWS])
            q_store(b).start()
            if with_kv:
                @pl.when(b == nq - 2)
                def _():
                    sends[0].wait_recv()
                    forward.start()

            return carry

        lax.fori_loop(0, nq, q_block, 0)
        for b in range(nq):
            q_store(b).wait()
        if with_kv:
            sends[0].wait_send()
            sends[1].wait()
            forward.wait()

    whole = lambda arr: pl.BlockSpec(arr.shape, lambda i: (0, 0))
    kv_shape = jax.ShapeDtypeStruct((rows, 2 * kv_cols), BF16)
    kv_out = [kv_shape] * 4 if with_kv else []
    return pl.pallas_call(
        kernel,
        grid=(1,),
        in_specs=[any_spec(), whole(gain), whole(pos2), whole(inv_freq), any_spec()] + [any_spec()] * (2 if with_kv else 0),
        out_specs=[any_spec()] + ([pl.BlockSpec(kv_shape.shape, lambda i: (0, 0)), any_spec(), any_spec(), any_spec()] if with_kv else []),
        out_shape=[jax.ShapeDtypeStruct((ROWS, q_cols), BF16)] + kv_out,
        scratch_shapes=[
            pltpu.VMEM((rows, d_model), BF16),
            pltpu.VMEM((rows, d_model), BF16),
            pltpu.VMEM((slots, deep, bn), BF16),
            pltpu.VMEM((ROWS, q_cols), BF16),
            pltpu.VMEM((rows, HEAD), F32),
            pltpu.VMEM((rows, HEAD), F32),
            pltpu.VMEM((1, HEAD), F32),
            pltpu.SemaphoreType.DMA((nx,)),
            pltpu.SemaphoreType.DMA((slots,)),
            pltpu.SemaphoreType.DMA((nq,)),
        ] + ([pltpu.SemaphoreType.DMA((3,))] * 2 if with_kv else []),
        compiler_params=pltpu.CompilerParams(vmem_limit_bytes=VMEM_BYTES, collective_id=group, has_side_effects=True) if with_kv else pltpu.CompilerParams(vmem_limit_bytes=VMEM_BYTES),
        cost_estimate=pl.CostEstimate(flops=2 * rows * d_model * (2 * kv_cols + q_cols), bytes_accessed=2 * d_model * (rows + q_cols), transcendentals=0),
        name="front",
    )(x_in, gain, pos2, inv_freq, w_q, *((w_k, w_v) if with_kv else ()))


def attend_send(row_group, cp_size, pos, pos2, q, kv_parts, w_o, cols):
    half = row_group // 2
    qb = kb = ROWS
    rows = 2 * ROWS
    kv_heads = kv_parts[0].shape[1] // (2 * HEAD)
    group = q.shape[1] // (kv_heads * HEAD)
    keys = cp_size * rows * (1 + half)
    scale = HEAD ** -0.5
    parts = len(kv_parts)
    k_dim = q.shape[1]
    half_cols = w_o.shape[1] // 2
    bn = 512
    unroll = 2 if row_group < 3 else 1

    def kernel(pos_ref, pos2_ref, q_hbm, w_hbm, *rest):
        kv_hbm = rest[:parts]
        o_hbm, part_hbm, kv_all, q_buf, o_buf, part_buf, w_buf, s_ref, p_ref, m_ref, l_ref, acc_ref, kv_sem, q_sem, w_sem, o_sem, p_sem = rest[parts:]
        dev, tp = lax.axis_index('cp'), lax.axis_index('tp')
        copies = []
        for n in range(parts):
            owner = lax.bitwise_xor(dev, n % cp_size)
            piece = owner if n < cp_size else 2 * cp_size - 1 - owner
            copies.append(pltpu.make_async_copy(kv_hbm[n], kv_all.at[pl.ds(pl.multiple_of(piece * rows, rows), rows)], kv_sem.at[n]))
            copies[-1].start()

        def q_copy(n):
            at = pl.ds(pl.multiple_of(n * group * HEAD, group * HEAD), group * HEAD)
            return pltpu.make_async_copy(q_hbm.at[:, at], q_buf.at[:, at], q_sem.at[n])

        for n in range(unroll):
            q_copy(n).start()

        def w_copy(j):
            at = pl.ds(pl.multiple_of((1 - tp) * half_cols + j * bn, bn), bn)
            return pltpu.make_async_copy(w_hbm.at[:, at], w_buf.at[j], w_sem.at[j])

        for copy in copies:
            copy.wait()
        for n in range(unroll, kv_heads):
            q_copy(n).start()
        for j in range(cols // bn):
            w_copy(j).start()
        piece = dev if half == 0 else 2 * cp_size - 1 - dev
        lane = lax.broadcasted_iota(jnp.int32, (qb, LANES), 1)
        t0 = piece * rows + (row_group % 2) * qb
        p0 = pos_ref[row_group * qb]
        t_idx = t0 + lax.broadcasted_iota(jnp.int32, (qb, LANES), 0)
        pos_row = pos2_ref[row_group:row_group + 1, :].astype(F32)
        first = t_idx - jnp.transpose(jnp.broadcast_to(pos_row, (qb, LANES))).astype(jnp.int32)

        def head_cols(n, g):
            return pl.ds(pl.multiple_of((n * group + g) * HEAD, HEAD), HEAD)

        def kv_cols(n):
            return pl.ds(pl.multiple_of(n * HEAD, HEAD), HEAD)

        def stack(n):
            return jnp.concatenate([q_buf[:, head_cols(n, g)] for g in range(group)], axis=0)

        @pl.when(p0 <= kb)
        def _():
            w0 = pl.multiple_of(jnp.maximum(t0 - kb, 0), kb)
            at = pl.ds(w0, 2 * kb)
            u = w0 + lane
            visible = jnp.concatenate([(u >= first) & (u <= t_idx), (u + kb >= first) & (u + kb <= t_idx)], axis=1)

            def some_heads(i, carry):
                for j in range(unroll):
                    n = i * unroll + j
                    q_copy(n).wait()
                    s_ref[j] = lax.dot_general(stack(n), kv_all[at, kv_cols(n)], (((1,), (1,)), ((), ())), preferred_element_type=F32)
                for j in range(unroll):
                    for g in range(group):
                        at_g = slice(g * qb, (g + 1) * qb)
                        s = jnp.where(visible, s_ref[j, at_g] * scale, -1e30)
                        s_ref[j, at_g] = s
                        m_ref[g] = jnp.broadcast_to(jnp.max(s, axis=1, keepdims=True), (qb, LANES))
                    for g in range(group):
                        at_g = slice(g * qb, (g + 1) * qb)
                        m = m_ref[g]
                        e = jnp.exp(s_ref[j, at_g] - jnp.concatenate([m, m], axis=1))
                        s_ref[j, at_g] = e
                        l_ref[g] = 1.0 / jnp.broadcast_to(jnp.sum(e, axis=1, keepdims=True), (qb, LANES))
                    for g in range(group):
                        at_g = slice(g * qb, (g + 1) * qb)
                        inv = l_ref[g]
                        p_ref[j, at_g] = (s_ref[j, at_g] * jnp.concatenate([inv, inv], axis=1)).astype(BF16)
                    n = i * unroll + j
                    o = jnp.dot(p_ref[j], kv_all[at, kv_cols(kv_heads + n)], preferred_element_type=F32).astype(BF16)
                    for g in range(group):
                        o_buf[:, head_cols(n, g)] = o[g * qb:(g + 1) * qb]
                return carry

            lax.fori_loop(0, kv_heads // unroll, some_heads, 0)

        @pl.when(p0 > kb)
        def _():
            kb0 = lax.div(t0 - p0, kb)
            kb1 = lax.div(t0, kb) + 1

            def kv_head(n, carry):
                q_copy(n).wait()
                q_stack = stack(n)
                m_ref[...] = jnp.full_like(m_ref, -1e30)
                l_ref[...] = jnp.zeros_like(l_ref)
                acc_ref[...] = jnp.zeros_like(acc_ref)

                def block(j):
                    at = pl.ds(pl.multiple_of(j * kb, kb), kb)
                    u = j * kb + lane
                    s_ref[0, :, :kb] = lax.dot_general(q_stack, kv_all[at, kv_cols(n)], (((1,), (1,)), ((), ())), preferred_element_type=F32)
                    return at, (u >= first) & (u <= t_idx)

                def head_scores(g, visible):
                    at_g = pl.ds(pl.multiple_of(g * qb, qb), qb)
                    return at_g, jnp.where(visible, s_ref[0, at_g, :kb] * scale, -1e30)

                def stats(j, inner):
                    _, visible = block(j)

                    def one(g, c):
                        _, s = head_scores(g, visible)
                        m_old = m_ref[g]
                        m_new = jnp.maximum(m_old, jnp.max(s, axis=1, keepdims=True))
                        l_ref[g] = l_ref[g] * jnp.exp(m_old - m_new) + jnp.sum(jnp.exp(s - m_new), axis=1, keepdims=True)
                        m_ref[g] = m_new
                        return c

                    return lax.fori_loop(0, group, one, inner)

                def weigh(j, inner):
                    at, visible = block(j)

                    def one(g, c):
                        at_g, s = head_scores(g, visible)
                        p_ref[0, at_g, :kb] = (jnp.exp(s - m_ref[g]) / l_ref[g]).astype(BF16)
                        return c

                    lax.fori_loop(0, group, one, 0)
                    acc_ref[...] += jnp.dot(p_ref[0, :, :kb], kv_all[at, kv_cols(kv_heads + n)], preferred_element_type=F32)
                    return inner

                lax.fori_loop(kb0, kb1, stats, 0)
                lax.fori_loop(kb0, kb1, weigh, 0)
                for g in range(group):
                    o_buf[:, head_cols(n, g)] = acc_ref[g * qb:(g + 1) * qb].astype(BF16)
                return carry

            lax.fori_loop(0, kv_heads, kv_head, 0)

        o_copy = pltpu.make_async_copy(o_buf, o_hbm, o_sem)
        o_copy.start()

        def part_copy(j):
            at = pl.ds(pl.multiple_of(j * bn, bn), bn)
            return pltpu.make_async_copy(part_buf.at[:, at], part_hbm.at[:, at], p_sem.at[j])

        def product(j, carry):
            w_copy(j).wait()
            part_buf[:, pl.ds(pl.multiple_of(j * bn, bn), bn)] = jnp.dot(o_buf[...], w_buf[j], preferred_element_type=F32)
            part_copy(j).start()
            return carry

        lax.fori_loop(0, cols // bn, product, 0)
        o_copy.wait()
        for j in range(cols // bn):
            part_copy(j).wait()

    whole = lambda shape: pl.BlockSpec(shape, lambda i, *_: (0, 0))
    return pl.pallas_call(
        kernel,
        grid_spec=pltpu.PrefetchScalarGridSpec(
            num_scalar_prefetch=1,
            grid=(1,),
            in_specs=[whole(pos2.shape), any_spec(), any_spec()] + [any_spec()] * parts,
            out_specs=[any_spec(), any_spec()],
            scratch_shapes=[
                pltpu.VMEM((keys, kv_parts[0].shape[1]), BF16),
                pltpu.VMEM(q.shape, BF16),
                pltpu.VMEM(q.shape, BF16),
                pltpu.VMEM((ROWS, cols), F32),
                pltpu.VMEM((cols // bn, k_dim, bn), BF16),
                pltpu.VMEM((unroll, group * qb, 2 * kb), F32),
                pltpu.VMEM((unroll, group * qb, 2 * kb), BF16),
                pltpu.VMEM((group, qb, LANES), F32),
                pltpu.VMEM((group, qb, LANES), F32),
                pltpu.VMEM((group * qb, HEAD), F32),
                pltpu.SemaphoreType.DMA((parts,)),
                pltpu.SemaphoreType.DMA((kv_heads,)),
                pltpu.SemaphoreType.DMA((cols // bn,)),
                pltpu.SemaphoreType.DMA,
                pltpu.SemaphoreType.DMA((cols // bn,)),
            ],
        ),
        out_shape=[jax.ShapeDtypeStruct(q.shape, BF16), jax.ShapeDtypeStruct((ROWS, cols), F32)],
        compiler_params=pltpu.CompilerParams(vmem_limit_bytes=VMEM_BYTES),
        cost_estimate=pl.CostEstimate(flops=4 * ROWS * k_dim * 512 + 2 * ROWS * k_dim * cols, bytes_accessed=2 * k_dim * cols, transcendentals=0),
        name="attend_send",
    )(pos, pos2, q, w_o, *kv_parts)


def out_cols(row_group, o, w_o, col0, cols, x_in=None, recvs=(), y_buf=None):
    rows, k_dim = o.shape
    bn = 512
    nb = cols // bn
    half_cols = w_o.shape[1] // 2
    own = bool(recvs)
    starts = [sum(r.shape[1] for r in recvs[:n]) for n in range(len(recvs))]

    def kernel(o_hbm, w_hbm, *rest):
        if own:
            x_hbm, recv_hbm = rest[0], rest[1:1 + len(recvs)]
            rest = rest[1 + len(recvs) + (y_buf is not None):]
            y_hbm, c_hbm, o_buf, w_buf, c_buf, o_sem, w_sem, c_sem, x_buf, r_buf, x_sem, r_sem, y_sem = rest
        else:
            c_hbm, o_buf, w_buf, c_buf, o_sem, w_sem, c_sem = rest
        tp = lax.axis_index('tp')
        side = tp if own else 1 - tp
        base = side * half_cols + col0

        def w_copy(j):
            return pltpu.make_async_copy(w_hbm.at[:, pl.ds(pl.multiple_of(base + j * bn, bn), bn)], w_buf.at[j], w_sem.at[j])

        def out_copies(j):
            at = pl.ds(pl.multiple_of(j * bn, bn), bn)
            copies = [pltpu.make_async_copy(c_buf.at[:, at], c_hbm.at[:, at], c_sem.at[j])]
            if own:
                to = y_hbm.at[pl.ds(row_group * ROWS, rows), pl.ds(pl.multiple_of(base + j * bn, bn), bn)]
                copies.append(pltpu.make_async_copy(c_buf.at[:, at], to, y_sem.at[j]))
            return copies

        o_copy = pltpu.make_async_copy(o_hbm, o_buf, o_sem)
        o_copy.start()
        w_copy(0).start()
        extra = []
        if own:
            extra.append(pltpu.make_async_copy(x_hbm.at[pl.ds(row_group * ROWS, rows), pl.ds(pl.multiple_of(base, bn), cols)], x_buf, x_sem))
            for n, recv in enumerate(recv_hbm):
                extra.append(pltpu.make_async_copy(recv, r_buf.at[:, starts[n]:starts[n] + recv.shape[1]], r_sem.at[n]))
            for copy in extra:
                copy.start()
        if nb > 1:
            w_copy(1).start()
        o_copy.wait()
        for copy in extra:
            copy.wait()

        def block(j, carry):
            at = pl.ds(pl.multiple_of(j * bn, bn), bn)
            w_copy(j).wait()

            @pl.when(j + 2 < nb)
            def _():
                w_copy(j + 2).start()

            acc = jnp.dot(o_buf[...], w_buf[j], preferred_element_type=F32)
            if own:
                c_buf[:, at] = (x_buf[:, at].astype(F32) + (acc + r_buf[:, at])).astype(BF16)
            else:
                c_buf[:, at] = acc
            for copy in out_copies(j):
                copy.start()
            return carry

        lax.fori_loop(0, nb, block, 0)

        def finish(j, carry):
            for copy in out_copies(j):
                copy.wait()
            return carry

        lax.fori_loop(0, nb, finish, 0)

    kind = BF16 if own else F32
    chunk = jax.ShapeDtypeStruct((rows, cols), kind)
    ins = [o, w_o] + ([x_in, *recvs] if own else []) + ([] if y_buf is None else [y_buf])
    sems = [pltpu.SemaphoreType.DMA, pltpu.SemaphoreType.DMA((nb,)), pltpu.SemaphoreType.DMA((nb,))]
    scratch = [pltpu.VMEM((rows, k_dim), BF16), pltpu.VMEM((nb, k_dim, bn), BF16), pltpu.VMEM((rows, cols), kind)] + sems
    if own:
        scratch += [pltpu.VMEM((rows, cols), BF16), pltpu.VMEM((rows, cols), F32), pltpu.SemaphoreType.DMA, pltpu.SemaphoreType.DMA((len(recvs),)), pltpu.SemaphoreType.DMA((nb,))]
    return pl.pallas_call(
        kernel,
        grid=(1,),
        in_specs=[any_spec()] * len(ins),
        out_specs=[any_spec()] * (2 if own else 1),
        out_shape=([jax.ShapeDtypeStruct(x_in.shape, BF16)] if own else []) + [chunk],
        scratch_shapes=scratch,
        input_output_aliases={} if y_buf is None else {len(ins) - 1: 0},
        compiler_params=pltpu.CompilerParams(vmem_limit_bytes=VMEM_BYTES),
        cost_estimate=pl.CostEstimate(flops=2 * rows * k_dim * cols, bytes_accessed=2 * k_dim * (rows + cols), transcendentals=0),
        name="out_own" if own else "out_send",
    )(*ins)


def place(row_group, tp_me, recv, y_buf, col0):
    rows, cols = recv.shape
    half_cols = y_buf.shape[1] // 2
    bn = min(cols, 2048)

    def kernel(tp_ref, r_ref, y_in, y_ref):
        y_ref[...] = r_ref[...]

    return pl.pallas_call(
        kernel,
        grid_spec=pltpu.PrefetchScalarGridSpec(
            num_scalar_prefetch=1,
            grid=(cols // bn,),
            in_specs=[pl.BlockSpec((rows, bn), lambda i, tp: (0, i)), any_spec()],
            out_specs=pl.BlockSpec((rows, bn), lambda i, tp: (row_group, ((1 - tp[0]) * half_cols + col0) // bn + i)),
        ),
        out_shape=jax.ShapeDtypeStruct(y_buf.shape, BF16),
        input_output_aliases={2: 0},
        compiler_params=pltpu.CompilerParams(vmem_limit_bytes=8 * 1024 * 1024),
        cost_estimate=pl.CostEstimate(flops=rows * cols, bytes_accessed=4 * rows * cols, transcendentals=0),
        name="place",
    )(tp_me, recv, y_buf)


def solution(mesh):
    cp_size = mesh.shape['cp']
    tp_size = mesh.shape['tp']
    swap_tp = [(j, tp_size - 1 - j) for j in range(tp_size)]

    def local_step(x_in, doc_id, pos_in_doc, norm_gain, w_q, w_k, w_v, w_o, inv_freq):
        local_rows, d_model = x_in.shape
        kv_cols = w_k.shape[1]
        groups = local_rows // ROWS
        tp_me = lax.axis_index('tp').astype(jnp.int32).reshape(1)
        gain = norm_gain.reshape(1, d_model)
        pos2 = pos_in_doc.reshape(groups, LANES)
        freq = inv_freq.reshape(1, HEAD // 2)
        kv_parts = []
        attn, sent, results = {}, {}, []
        y_buf = None

        def swap(value):
            return lax.ppermute(value, 'tp', swap_tp)

        def make(r):
            q, *parts = front(r, r % 2 == 0, x_in, gain, pos2, freq, w_q, w_k, w_v)
            kv_parts.extend(parts)
            sizes = CHUNKS[r]
            attn[r], part = attend_send(r, cp_size, pos_in_doc, pos2, q, kv_parts, w_o, sizes[0])
            sent[r] = [swap(part)]
            for c in range(1, len(sizes)):
                part, = out_cols(r, attn[r], w_o, sum(sizes[:c]), sizes[c])
                sent[r].append(swap(part))

        for kind, r, c0, c1 in PLAN:
            if kind == "make":
                make(r)
                continue
            col0 = sum(CHUNKS[r][:c0])
            y_buf, block = out_cols(r, attn[r], w_o, col0, sum(CHUNKS[r][c0:c1]), x_in, sent[r][c0:c1], y_buf)
            results.append((r, col0, swap(block)))
        for r, col0, block in results:
            y_buf = place(r, tp_me, block, y_buf, col0)
        kv_all = jnp.concatenate([kv_parts[0], kv_parts[cp_size]], axis=0)
        k_out = kv_all[:, :kv_cols].reshape(local_rows, kv_cols // HEAD, HEAD)
        v_out = kv_all[:, kv_cols:].reshape(local_rows, kv_cols // HEAD, HEAD)
        return y_buf, k_out, v_out

    row_spec = P(('dp', 'cp'))
    in_specs = (P(('dp', 'cp'), None), row_spec, row_spec, P(), P(None, 'tp'), P(None, 'tp'), P(None, 'tp'), P('tp', None), P())
    out_specs = (P(('dp', 'cp'), None), P(('dp', 'cp'), 'tp', None), P(('dp', 'cp'), 'tp', None))

    return jax.shard_map(local_step, mesh=mesh, in_specs=in_specs, out_specs=out_specs, check_vma=False)
```

```python
import jax
import jax.numpy as jnp
from jax import lax
from jax.experimental import pallas as pl
from jax.experimental.pallas import tpu as pltpu
from jax.sharding import PartitionSpec as P


F32 = jnp.float32
BF16 = jnp.bfloat16
HEAD = 128
LANES = 128
VMEM_BYTES = 67043328
ROWS = 128
CHUNKS = ((1024, 3072), (1024, 3072), (1024, 3072), (2048, 1024, 512, 512))
PLAN = (("make", 0, 0, 2), ("make", 1, 0, 2), ("own", 0, 0, 2), ("make", 2, 0, 2), ("own", 1, 0, 2), ("make", 3, 0, 4), ("own", 2, 0, 2), ("own", 3, 0, 1), ("own", 3, 1, 2), ("own", 3, 2, 3), ("own", 3, 3, 4))


def any_spec():
    return pl.BlockSpec(memory_space=pl.ANY)


def rope_head(vec, cos_t, sin_t):
    vec = vec.astype(BF16).astype(F32)
    return (vec * cos_t + pltpu.roll(vec, HEAD // 2, 1) * sin_t).astype(BF16)


def front(group, with_kv, x_in, gain, pos2, inv_freq, w_q, w_k, w_v):
    d_model = x_in.shape[1]
    kv_cols = w_k.shape[1]
    q_cols = w_q.shape[1]
    bn = kv_cols
    nq = q_cols // bn
    slots = 8
    ahead = 4
    deep = d_model // 2
    xr = 64
    rows = 2 * ROWS if with_kv else ROWS
    nx = rows // xr
    step = 16
    lead = 4 if with_kv else 0

    def kernel(x_hbm, gain_hbm, pos_hbm, freq_hbm, wq_hbm, *rest):
        if with_kv:
            wk_hbm, wv_hbm, q_hbm, kv_hbm, r1, r2, r3 = rest[:7]
            kv_ref, kv_sem, s_sem, r_sem = rest[-4:]
            rest = rest[7:-4]
            kv_store = pltpu.make_async_copy(kv_ref, kv_hbm, kv_sem)
            me = lax.axis_index('cp')
            core, across = lax.bitwise_xor(me, 1), lax.bitwise_xor(me, 2)
            barrier = pltpu.get_barrier_semaphore()
            for peer in (core, across):
                pl.semaphore_signal(barrier, inc=1, device_id={'cp': peer}, device_id_type=pl.DeviceIdType.MESH)
        else:
            q_hbm = rest[0]
            rest = rest[1:]
        x_buf, h_ref, ring, q_buf, cos_ref, sin_ref, freq2_ref, gain_ref, pos_ref, freq_ref, x_sem, w_sem, q_sem, small_sem = rest
        small = [pltpu.make_async_copy(src, dst, small_sem.at[n]) for n, (src, dst) in enumerate(((pos_hbm, pos_ref), (freq_hbm, freq_ref), (gain_hbm, gain_ref)))]
        for copy in small:
            copy.start()
        x_copies = [pltpu.make_async_copy(x_hbm.at[pl.ds(group * ROWS + i * xr, xr)], x_buf.at[pl.ds(i * xr, xr)], x_sem.at[i]) for i in range(nx)]
        for copy in x_copies:
            copy.start()

        def q_load(b, part):
            slot = lax.rem(2 * b + part + lead, slots)
            return pltpu.make_async_copy(wq_hbm.at[pl.ds(part * deep, deep), pl.ds(pl.multiple_of(b * bn, bn), bn)], ring.at[slot], w_sem.at[slot])

        def load(u):
            if u >= lead:
                return q_load((u - lead) // 2, u % 2)
            w_hbm = (wk_hbm, wv_hbm)[u // 2]
            return pltpu.make_async_copy(w_hbm.at[pl.ds((u % 2) * deep, deep)], ring.at[u], w_sem.at[u])

        load(0).start()
        load(1).start()

        for copy in small:
            copy.wait()
        half_dim = HEAD // 2
        freq2_ref[:, :half_dim] = freq_ref[...]
        freq2_ref[:, half_dim:] = freq_ref[...]
        sign = jnp.where(lax.broadcasted_iota(jnp.int32, (LANES, HEAD), 1) < half_dim, -1.0, 1.0)
        for b in range(rows // LANES):
            pos_row = pos_ref[group + b:group + b + 1, :].astype(F32)
            angle = jnp.transpose(jnp.broadcast_to(pos_row, (LANES, LANES))) * freq2_ref[...]
            cos_ref[b * LANES:(b + 1) * LANES, :] = jnp.cos(angle)
            sin_ref[b * LANES:(b + 1) * LANES, :] = jnp.sin(angle) * sign

        def norm(r, carry):
            at = pl.ds(pl.multiple_of(r * step, step), step)
            total = jnp.zeros((step, LANES), F32)
            for c in range(d_model // LANES):
                v = x_buf[at, c * LANES:(c + 1) * LANES].astype(F32)
                total += v * v
            inv = lax.rsqrt(jnp.sum(total, axis=1, keepdims=True) / d_model + 1e-5)
            for c in range(d_model // LANES):
                cols = slice(c * LANES, (c + 1) * LANES)
                h_ref[at, cols] = (x_buf[at, cols].astype(F32) * inv * gain_ref[:, cols]).astype(BF16)
            return carry

        for i in range(nx):
            x_copies[i].wait()
        load(2).start()
        load(3).start()
        lax.fori_loop(0, rows // step, norm, 0)

        def product(lhs_rows, slots_of, waits, after):
            acc = None
            for part in range(2):
                waits(part)
                after(part)
                half_acc = jnp.dot(h_ref[:lhs_rows, part * deep:(part + 1) * deep], ring[slots_of(part)], preferred_element_type=F32)
                acc = half_acc if acc is None else acc + half_acc
            return acc

        if with_kv:
            for n in range(2):
                acc = product(rows, lambda part: 2 * n + part, lambda part: load(2 * n + part).wait(), lambda part: load(2 * n + part + ahead).start())
                for g in range(bn // HEAD):
                    cols = slice(g * HEAD, (g + 1) * HEAD)
                    to = slice(n * kv_cols + g * HEAD, n * kv_cols + (g + 1) * HEAD)
                    kv_ref[:, to] = rope_head(acc[:, cols], cos_ref[...], sin_ref[...]) if n == 0 else acc[:, cols].astype(BF16)
            pl.semaphore_wait(barrier, 2)
            kv_store.start()
            sends = []
            for n, (dst, peer) in enumerate(((r2, across), (r1, core))):
                sends.append(pltpu.make_async_remote_copy(src_ref=kv_ref, dst_ref=dst, send_sem=s_sem.at[n], recv_sem=r_sem.at[n], device_id={'cp': peer}, device_id_type=pl.DeviceIdType.MESH))
                sends[-1].start()
            forward = pltpu.make_async_remote_copy(src_ref=r2, dst_ref=r3, send_sem=s_sem.at[2], recv_sem=r_sem.at[2], device_id={'cp': core}, device_id_type=pl.DeviceIdType.MESH)

        def q_store(b):
            cols = pl.ds(pl.multiple_of(b * bn, bn), bn)
            return pltpu.make_async_copy(q_buf.at[:, cols], q_hbm.at[:, cols], q_sem.at[b])

        def q_block(b, carry):
            def after(part):
                @pl.when(b + ahead // 2 < nq)
                def _():
                    q_load(b + ahead // 2, part).start()

            acc = product(ROWS, lambda part: lax.rem(2 * b + part + lead, slots), lambda part: q_load(b, part).wait(), after)
            for g in range(bn // HEAD):
                at = pl.ds(pl.multiple_of(b * bn + g * HEAD, HEAD), HEAD)
                q_buf[:, at] = rope_head(acc[:, g * HEAD:(g + 1) * HEAD], cos_ref[:ROWS], sin_ref[:ROWS])
            q_store(b).start()
            if with_kv:
                @pl.when(b == nq - 2)
                def _():
                    sends[0].wait_recv()
                    forward.start()

            return carry

        lax.fori_loop(0, nq, q_block, 0)
        for b in range(nq):
            q_store(b).wait()
        if with_kv:
            kv_store.wait()
            sends[0].wait_send()
            sends[1].wait()
            forward.wait()

    kv_shape = jax.ShapeDtypeStruct((rows, 2 * kv_cols), BF16)
    kv_out = [kv_shape] * 4 if with_kv else []
    return pl.pallas_call(
        kernel,
        grid=(1,),
        in_specs=[any_spec()] * (7 if with_kv else 5),
        out_specs=[any_spec()] * (5 if with_kv else 1),
        out_shape=[jax.ShapeDtypeStruct((ROWS, q_cols), BF16)] + kv_out,
        scratch_shapes=[
            pltpu.VMEM((rows, d_model), BF16),
            pltpu.VMEM((rows, d_model), BF16),
            pltpu.VMEM((slots, deep, bn), BF16),
            pltpu.VMEM((ROWS, q_cols), BF16),
            pltpu.VMEM((rows, HEAD), F32),
            pltpu.VMEM((rows, HEAD), F32),
            pltpu.VMEM((1, HEAD), F32),
            pltpu.VMEM(gain.shape, F32),
            pltpu.VMEM(pos2.shape, jnp.int32),
            pltpu.VMEM(inv_freq.shape, F32),
            pltpu.SemaphoreType.DMA((nx,)),
            pltpu.SemaphoreType.DMA((slots,)),
            pltpu.SemaphoreType.DMA((nq,)),
            pltpu.SemaphoreType.DMA((3,)),
        ] + ([pltpu.VMEM(kv_shape.shape, BF16), pltpu.SemaphoreType.DMA, pltpu.SemaphoreType.DMA((3,)), pltpu.SemaphoreType.DMA((3,))] if with_kv else []),
        compiler_params=pltpu.CompilerParams(vmem_limit_bytes=VMEM_BYTES, collective_id=group, has_side_effects=True) if with_kv else pltpu.CompilerParams(vmem_limit_bytes=VMEM_BYTES),
        cost_estimate=pl.CostEstimate(flops=2 * rows * d_model * (2 * kv_cols + q_cols), bytes_accessed=2 * d_model * (rows + q_cols), transcendentals=0),
        name="front",
    )(x_in, gain, pos2, inv_freq, w_q, *((w_k, w_v) if with_kv else ()))


def attend_send(row_group, cp_size, pos, pos2, q, kv_parts, w_o, cols):
    half = row_group // 2
    qb = kb = ROWS
    rows = 2 * ROWS
    kv_heads = kv_parts[0].shape[1] // (2 * HEAD)
    group = q.shape[1] // (kv_heads * HEAD)
    keys = cp_size * rows * (1 + half)
    scale = HEAD ** -0.5
    parts = len(kv_parts)
    k_dim = q.shape[1]
    half_cols = w_o.shape[1] // 2
    bn = 512
    unroll = (4, 2, 1, 1)[row_group]

    def kernel(pos_ref, pos2_hbm, q_hbm, w_hbm, *rest):
        kv_hbm = rest[:parts]
        o_hbm, part_hbm, pos2_ref, pos2_sem, kv_all, q_buf, o_buf, part_buf, w_buf, s_ref, p_ref, m_ref, l_ref, acc_ref, kv_sem, q_sem, w_sem, o_sem, p_sem = rest[parts:]
        dev, tp = lax.axis_index('cp'), lax.axis_index('tp')
        copies = [pltpu.make_async_copy(pos2_hbm, pos2_ref, pos2_sem)]
        copies[0].start()
        for n in range(parts):
            owner = lax.bitwise_xor(dev, n % cp_size)
            piece = owner if n < cp_size else 2 * cp_size - 1 - owner
            copies.append(pltpu.make_async_copy(kv_hbm[n], kv_all.at[pl.ds(pl.multiple_of(piece * rows, rows), rows)], kv_sem.at[n]))
            copies[-1].start()

        def q_copy(n):
            at = pl.ds(pl.multiple_of(n * group * HEAD, group * HEAD), group * HEAD)
            return pltpu.make_async_copy(q_hbm.at[:, at], q_buf.at[:, at], q_sem.at[n])

        for n in range(unroll):
            q_copy(n).start()

        def w_copy(j):
            at = pl.ds(pl.multiple_of((1 - tp) * half_cols + j * bn, bn), bn)
            return pltpu.make_async_copy(w_hbm.at[:, at], w_buf.at[j], w_sem.at[j])

        for copy in copies:
            copy.wait()
        for n in range(unroll, kv_heads):
            q_copy(n).start()
        for j in range(cols // bn):
            w_copy(j).start()
        piece = dev if half == 0 else 2 * cp_size - 1 - dev
        lane = lax.broadcasted_iota(jnp.int32, (qb, LANES), 1)
        t0 = piece * rows + (row_group % 2) * qb
        p0 = pos_ref[row_group * qb]
        t_idx = t0 + lax.broadcasted_iota(jnp.int32, (qb, LANES), 0)
        pos_row = pos2_ref[row_group:row_group + 1, :].astype(F32)
        first = t_idx - jnp.transpose(jnp.broadcast_to(pos_row, (qb, LANES))).astype(jnp.int32)

        def head_cols(n, g):
            return pl.ds(pl.multiple_of((n * group + g) * HEAD, HEAD), HEAD)

        def kv_cols(n):
            return pl.ds(pl.multiple_of(n * HEAD, HEAD), HEAD)

        def stack(n):
            return jnp.concatenate([q_buf[:, head_cols(n, g)] for g in range(group)], axis=0)

        @pl.when(p0 <= kb)
        def _():
            w0 = pl.multiple_of(jnp.maximum(t0 - kb, 0), kb)
            at = pl.ds(w0, 2 * kb)
            u = w0 + lane
            visible = jnp.concatenate([(u >= first) & (u <= t_idx), (u + kb >= first) & (u + kb <= t_idx)], axis=1)

            def some_heads(i, carry):
                for j in range(unroll):
                    n = i * unroll + j
                    q_copy(n).wait()
                    s_ref[j] = lax.dot_general(stack(n), kv_all[at, kv_cols(n)], (((1,), (1,)), ((), ())), preferred_element_type=F32)
                for j in range(unroll):
                    for g in range(group):
                        at_g = slice(g * qb, (g + 1) * qb)
                        s = jnp.where(visible, s_ref[j, at_g] * scale, -1e30)
                        s_ref[j, at_g] = s
                        m_ref[g] = jnp.broadcast_to(jnp.max(s, axis=1, keepdims=True), (qb, LANES))
                    for g in range(group):
                        at_g = slice(g * qb, (g + 1) * qb)
                        m = m_ref[g]
                        e = jnp.exp(s_ref[j, at_g] - jnp.concatenate([m, m], axis=1))
                        s_ref[j, at_g] = e
                        l_ref[g] = 1.0 / jnp.broadcast_to(jnp.sum(e, axis=1, keepdims=True), (qb, LANES))
                    for g in range(group):
                        at_g = slice(g * qb, (g + 1) * qb)
                        inv = l_ref[g]
                        p_ref[j, at_g] = (s_ref[j, at_g] * jnp.concatenate([inv, inv], axis=1)).astype(BF16)
                    n = i * unroll + j
                    o = jnp.dot(p_ref[j], kv_all[at, kv_cols(kv_heads + n)], preferred_element_type=F32).astype(BF16)
                    for g in range(group):
                        o_buf[:, head_cols(n, g)] = o[g * qb:(g + 1) * qb]
                return carry

            lax.fori_loop(0, kv_heads // unroll, some_heads, 0)

        @pl.when(p0 > kb)
        def _():
            kb0 = lax.div(t0 - p0, kb)
            kb1 = lax.div(t0, kb) + 1

            def kv_head(n, carry):
                q_copy(n).wait()
                q_stack = stack(n)
                m_ref[...] = jnp.full_like(m_ref, -1e30)
                l_ref[...] = jnp.zeros_like(l_ref)
                acc_ref[...] = jnp.zeros_like(acc_ref)

                def block(j):
                    at = pl.ds(pl.multiple_of(j * kb, kb), kb)
                    u = j * kb + lane
                    s_ref[0, :, :kb] = lax.dot_general(q_stack, kv_all[at, kv_cols(n)], (((1,), (1,)), ((), ())), preferred_element_type=F32)
                    return at, (u >= first) & (u <= t_idx)

                def head_scores(g, visible):
                    at_g = pl.ds(pl.multiple_of(g * qb, qb), qb)
                    return at_g, jnp.where(visible, s_ref[0, at_g, :kb] * scale, -1e30)

                def stats(j, inner):
                    _, visible = block(j)

                    def one(g, c):
                        _, s = head_scores(g, visible)
                        m_old = m_ref[g]
                        m_new = jnp.maximum(m_old, jnp.max(s, axis=1, keepdims=True))
                        l_ref[g] = l_ref[g] * jnp.exp(m_old - m_new) + jnp.sum(jnp.exp(s - m_new), axis=1, keepdims=True)
                        m_ref[g] = m_new
                        return c

                    return lax.fori_loop(0, group, one, inner)

                def weigh(j, inner):
                    at, visible = block(j)

                    def one(g, c):
                        at_g, s = head_scores(g, visible)
                        p_ref[0, at_g, :kb] = (jnp.exp(s - m_ref[g]) / l_ref[g]).astype(BF16)
                        return c

                    lax.fori_loop(0, group, one, 0)
                    acc_ref[...] += jnp.dot(p_ref[0, :, :kb], kv_all[at, kv_cols(kv_heads + n)], preferred_element_type=F32)
                    return inner

                lax.fori_loop(kb0, kb1, stats, 0)
                lax.fori_loop(kb0, kb1, weigh, 0)
                for g in range(group):
                    o_buf[:, head_cols(n, g)] = acc_ref[g * qb:(g + 1) * qb].astype(BF16)
                return carry

            lax.fori_loop(0, kv_heads, kv_head, 0)

        o_copy = pltpu.make_async_copy(o_buf, o_hbm, o_sem)
        o_copy.start()

        def part_copy(j):
            at = pl.ds(pl.multiple_of(j * bn, bn), bn)
            return pltpu.make_async_copy(part_buf.at[:, at], part_hbm.at[:, at], p_sem.at[j])

        def product(j, carry):
            w_copy(j).wait()
            part_buf[:, pl.ds(pl.multiple_of(j * bn, bn), bn)] = jnp.dot(o_buf[...], w_buf[j], preferred_element_type=F32)
            part_copy(j).start()
            return carry

        lax.fori_loop(0, cols // bn, product, 0)
        o_copy.wait()
        for j in range(cols // bn):
            part_copy(j).wait()

    return pl.pallas_call(
        kernel,
        grid_spec=pltpu.PrefetchScalarGridSpec(
            num_scalar_prefetch=1,
            grid=(1,),
            in_specs=[any_spec()] * (3 + parts),
            out_specs=[any_spec(), any_spec()],
            scratch_shapes=[
                pltpu.VMEM(pos2.shape, jnp.int32),
                pltpu.SemaphoreType.DMA,
                pltpu.VMEM((keys, kv_parts[0].shape[1]), BF16),
                pltpu.VMEM(q.shape, BF16),
                pltpu.VMEM(q.shape, BF16),
                pltpu.VMEM((ROWS, cols), F32),
                pltpu.VMEM((cols // bn, k_dim, bn), BF16),
                pltpu.VMEM((unroll, group * qb, 2 * kb), F32),
                pltpu.VMEM((unroll, group * qb, 2 * kb), BF16),
                pltpu.VMEM((group, qb, LANES), F32),
                pltpu.VMEM((group, qb, LANES), F32),
                pltpu.VMEM((group * qb, HEAD), F32),
                pltpu.SemaphoreType.DMA((parts,)),
                pltpu.SemaphoreType.DMA((kv_heads,)),
                pltpu.SemaphoreType.DMA((cols // bn,)),
                pltpu.SemaphoreType.DMA,
                pltpu.SemaphoreType.DMA((cols // bn,)),
            ],
        ),
        out_shape=[jax.ShapeDtypeStruct(q.shape, BF16), jax.ShapeDtypeStruct((ROWS, cols), F32)],
        compiler_params=pltpu.CompilerParams(vmem_limit_bytes=VMEM_BYTES),
        cost_estimate=pl.CostEstimate(flops=4 * ROWS * k_dim * 512 + 2 * ROWS * k_dim * cols, bytes_accessed=2 * k_dim * cols, transcendentals=0),
        name="attend_send",
    )(pos, pos2, q, w_o, *kv_parts)


def out_cols(row_group, o, w_o, col0, cols, x_in=None, recvs=(), y_buf=None):
    rows, k_dim = o.shape
    bn = 512
    nb = cols // bn
    half_cols = w_o.shape[1] // 2
    own = bool(recvs)
    starts = [sum(r.shape[1] for r in recvs[:n]) for n in range(len(recvs))]

    def kernel(o_hbm, w_hbm, *rest):
        if own:
            x_hbm, recv_hbm = rest[0], rest[1:1 + len(recvs)]
            rest = rest[1 + len(recvs) + (y_buf is not None):]
            y_hbm, c_hbm, o_buf, w_buf, c_buf, o_sem, w_sem, c_sem, x_buf, r_buf, x_sem, r_sem, y_sem = rest
        else:
            c_hbm, o_buf, w_buf, c_buf, o_sem, w_sem, c_sem = rest
        tp = lax.axis_index('tp')
        side = tp if own else 1 - tp
        base = side * half_cols + col0

        def w_copy(j):
            return pltpu.make_async_copy(w_hbm.at[:, pl.ds(pl.multiple_of(base + j * bn, bn), bn)], w_buf.at[j], w_sem.at[j])

        def out_copies(j):
            at = pl.ds(pl.multiple_of(j * bn, bn), bn)
            copies = [pltpu.make_async_copy(c_buf.at[:, at], c_hbm.at[:, at], c_sem.at[j])]
            if own:
                to = y_hbm.at[pl.ds(row_group * ROWS, rows), pl.ds(pl.multiple_of(base + j * bn, bn), bn)]
                copies.append(pltpu.make_async_copy(c_buf.at[:, at], to, y_sem.at[j]))
            return copies

        o_copy = pltpu.make_async_copy(o_hbm, o_buf, o_sem)
        o_copy.start()
        w_copy(0).start()
        extra = []
        if own:
            extra.append(pltpu.make_async_copy(x_hbm.at[pl.ds(row_group * ROWS, rows), pl.ds(pl.multiple_of(base, bn), cols)], x_buf, x_sem))
            for n, recv in enumerate(recv_hbm):
                extra.append(pltpu.make_async_copy(recv, r_buf.at[:, starts[n]:starts[n] + recv.shape[1]], r_sem.at[n]))
            for copy in extra:
                copy.start()
        if nb > 1:
            w_copy(1).start()
        o_copy.wait()
        for copy in extra:
            copy.wait()

        def block(j, carry):
            at = pl.ds(pl.multiple_of(j * bn, bn), bn)
            w_copy(j).wait()

            @pl.when(j + 2 < nb)
            def _():
                w_copy(j + 2).start()

            acc = jnp.dot(o_buf[...], w_buf[j], preferred_element_type=F32)
            if own:
                c_buf[:, at] = (x_buf[:, at].astype(F32) + (acc + r_buf[:, at])).astype(BF16)
            else:
                c_buf[:, at] = acc
            for copy in out_copies(j):
                copy.start()
            return carry

        lax.fori_loop(0, nb, block, 0)

        def finish(j, carry):
            for copy in out_copies(j):
                copy.wait()
            return carry

        lax.fori_loop(0, nb, finish, 0)

    kind = BF16 if own else F32
    chunk = jax.ShapeDtypeStruct((rows, cols), kind)
    ins = [o, w_o] + ([x_in, *recvs] if own else []) + ([] if y_buf is None else [y_buf])
    sems = [pltpu.SemaphoreType.DMA, pltpu.SemaphoreType.DMA((nb,)), pltpu.SemaphoreType.DMA((nb,))]
    scratch = [pltpu.VMEM((rows, k_dim), BF16), pltpu.VMEM((nb, k_dim, bn), BF16), pltpu.VMEM((rows, cols), kind)] + sems
    if own:
        scratch += [pltpu.VMEM((rows, cols), BF16), pltpu.VMEM((rows, cols), F32), pltpu.SemaphoreType.DMA, pltpu.SemaphoreType.DMA((len(recvs),)), pltpu.SemaphoreType.DMA((nb,))]
    return pl.pallas_call(
        kernel,
        grid=(1,),
        in_specs=[any_spec()] * len(ins),
        out_specs=[any_spec()] * (2 if own else 1),
        out_shape=([jax.ShapeDtypeStruct(x_in.shape, BF16)] if own else []) + [chunk],
        scratch_shapes=scratch,
        input_output_aliases={} if y_buf is None else {len(ins) - 1: 0},
        compiler_params=pltpu.CompilerParams(vmem_limit_bytes=VMEM_BYTES),
        cost_estimate=pl.CostEstimate(flops=2 * rows * k_dim * cols, bytes_accessed=2 * k_dim * (rows + cols), transcendentals=0),
        name="out_own" if own else "out_send",
    )(*ins)


def place(row_group, tp_me, recv, y_buf, col0):
    rows, cols = recv.shape
    half_cols = y_buf.shape[1] // 2
    bn = min(cols, 2048)

    def kernel(tp_ref, r_ref, y_in, y_ref):
        y_ref[...] = r_ref[...]

    return pl.pallas_call(
        kernel,
        grid_spec=pltpu.PrefetchScalarGridSpec(
            num_scalar_prefetch=1,
            grid=(cols // bn,),
            in_specs=[pl.BlockSpec((rows, bn), lambda i, tp: (0, i)), any_spec()],
            out_specs=pl.BlockSpec((rows, bn), lambda i, tp: (row_group, ((1 - tp[0]) * half_cols + col0) // bn + i)),
        ),
        out_shape=jax.ShapeDtypeStruct(y_buf.shape, BF16),
        input_output_aliases={2: 0},
        compiler_params=pltpu.CompilerParams(vmem_limit_bytes=8 * 1024 * 1024),
        cost_estimate=pl.CostEstimate(flops=rows * cols, bytes_accessed=4 * rows * cols, transcendentals=0),
        name="place",
    )(tp_me, recv, y_buf)


def solution(mesh):
    cp_size = mesh.shape['cp']
    tp_size = mesh.shape['tp']
    swap_tp = [(j, tp_size - 1 - j) for j in range(tp_size)]

    def local_step(x_in, doc_id, pos_in_doc, norm_gain, w_q, w_k, w_v, w_o, inv_freq):
        local_rows, d_model = x_in.shape
        kv_cols = w_k.shape[1]
        groups = local_rows // ROWS
        tp_me = lax.axis_index('tp').astype(jnp.int32).reshape(1)
        gain = norm_gain.reshape(1, d_model)
        pos2 = pos_in_doc.reshape(groups, LANES)
        freq = inv_freq.reshape(1, HEAD // 2)
        kv_parts = []
        attn, sent, results = {}, {}, []
        y_buf = None

        def swap(value):
            return lax.ppermute(value, 'tp', swap_tp)

        def make(r):
            q, *parts = front(r, r % 2 == 0, x_in, gain, pos2, freq, w_q, w_k, w_v)
            kv_parts.extend(parts)
            sizes = CHUNKS[r]
            attn[r], part = attend_send(r, cp_size, pos_in_doc, pos2, q, kv_parts, w_o, sizes[0])
            sent[r] = [swap(part)]
            for c in range(1, len(sizes)):
                part, = out_cols(r, attn[r], w_o, sum(sizes[:c]), sizes[c])
                sent[r].append(swap(part))

        for kind, r, c0, c1 in PLAN:
            if kind == "make":
                make(r)
                continue
            col0 = sum(CHUNKS[r][:c0])
            y_buf, block = out_cols(r, attn[r], w_o, col0, sum(CHUNKS[r][c0:c1]), x_in, sent[r][c0:c1], y_buf)
            results.append((r, col0, swap(block)))
        for r, col0, block in results:
            y_buf = place(r, tp_me, block, y_buf, col0)
        kv_all = jnp.concatenate([kv_parts[0], kv_parts[cp_size]], axis=0)
        k_out = kv_all[:, :kv_cols].reshape(local_rows, kv_cols // HEAD, HEAD)
        v_out = kv_all[:, kv_cols:].reshape(local_rows, kv_cols // HEAD, HEAD)
        return y_buf, k_out, v_out

    row_spec = P(('dp', 'cp'))
    in_specs = (P(('dp', 'cp'), None), row_spec, row_spec, P(), P(None, 'tp'), P(None, 'tp'), P(None, 'tp'), P('tp', None), P())
    out_specs = (P(('dp', 'cp'), None), P(('dp', 'cp'), 'tp', None), P(('dp', 'cp'), 'tp', None))

    return jax.shard_map(local_step, mesh=mesh, in_specs=in_specs, out_specs=out_specs, check_vma=False)
```
